32 devices in a mesh: section: 2 (over y), shard: 16 (over z, x, core).
Axes of the slice: x: 2, y: 2, z: 4, core: 2. Of those that a mesh axis runs over, the one named last changes fastest.
Arguments:
- section_input: bfloat16 [4, 16, 196, 256], P(None, 'shard'), may hold values from -6 to 6
- conv_one: bfloat16 [2, 2304, 256], P('section'), may hold values from -0.125 to 0.125
- conv_two: bfloat16 [2, 2304, 256], P('section'), may hold values from -0.125 to 0.125
- unit_gain: float32 [2, 256], P('section'), may hold values from 0.5 to 1.5
- offset_bias: float32 [2, 256], P('section'), may hold values from -3 to 3
- leak_slope: float32 [2, 256], P('section'), may hold values from 0.1 to 0.4
- depthwise: bfloat16 [196, 256], replicated, may hold values from -0.4375 to 0.4375
- embed_weight: bfloat16 [256, 512], replicated, may hold values from -0.375 to 0.375
- class_centers: bfloat16 [26624, 512], P('shard'), may hold values from -6 to 6
- labels: int32 [4, 16], replicated, may hold values from 0 to 26623
- class_offsets: int32 [16], P('shard'), may hold values from 0 to 24960, as said below
Outputs:
- section_grads: bfloat16 [2, 4, 16, 196, 256], P('section', None, 'shard')
The draws below stay inside these ranges and needn't reach their ends.
Inputs may be any that keep to these rules, and one draw needn't show every extreme that they name: `class_offsets`: each entry is 1664 times a different number of 0 to 15, so the blocks of class_centers hold every class of 0 to 26623 once.
All inputs are finite; a program needn't handle non-finite values.
Results may differ from the reference program's by a relative error of at most 0.03.
Values may be sent and summed in bfloat16 or wider, within the bound.
A program may use at most 64 MiB of HBM per device.

```python
import math
import jax
import jax.numpy as jnp
from jax import lax

C = 256
EMB = 512
SIDE = 14
CLS_DEV = 1664
MICRO = 4
FACES = 16
CLASSES = 26624
N_SECTION = 2
N_SHARD = 16


def draw_class_offsets(key, part):
    order = jax.random.permutation(jax.random.fold_in(key, 17), N_SHARD)
    return (order * CLS_DEV).astype(jnp.int32)


def plant(entries, own_key, low, top_value):
    longest = entries.shape.index(max(entries.shape))
    spots = []
    for shift in (0, 1):
        where = [jax.random.randint(jax.random.fold_in(own_key, axis), (), 0, length) for axis, length in enumerate(entries.shape)]
        where[longest] = (where[longest] + shift) % entries.shape[longest]
        spots.append(tuple(where))
    return entries.at[spots[0]].set(low).at[spots[1]].set(top_value)


def levels(own_key, extent, cuts, low, largest):
    def one(position, shards_of):
        draws = jax.random.uniform(jax.random.fold_in(jax.random.fold_in(own_key, 6), position), (shards_of,), jnp.float32, low / len(cuts), largest / len(cuts))
        return jnp.repeat(jnp.exp(draws), extent[position] // shards_of).reshape((-1,) + (1,) * (len(extent) - position - 1))

    gain = one(*cuts[0])
    for cut in cuts[1:]:
        gain = gain * one(*cut)
    return gain


def scatter_about(stream_key, extent, deviation, most, split=(), kind=jnp.bfloat16):
    factor_of = levels(stream_key, extent, split, -0.22, 0.18) if split else 1.0
    values = jax.random.normal(stream_key, extent, jnp.float32) * deviation * factor_of
    return jnp.minimum(jnp.maximum(values, -most), most).astype(kind)


def setup_inputs(seed: int = 0) -> dict:
    key_of = jax.random.split(jax.random.key(seed), 12)
    return {
        "section_input": scatter_about(key_of[0], (MICRO, FACES, SIDE * SIDE, C), 1.0, 6.0, ((1, 16),)),
        "conv_one": scatter_about(key_of[1], (N_SECTION, 9 * C, C), (9 * C) ** -0.5, 0.125, ((0, 2),)),
        "conv_two": scatter_about(key_of[2], (N_SECTION, 9 * C, C), (9 * C) ** -0.5, 0.125, ((0, 2),)),
        "unit_gain": jnp.clip(1.0 + 0.1 * jax.random.normal(key_of[3], (N_SECTION, C), jnp.float32), 0.5, 1.5),
        "offset_bias": scatter_about(key_of[4], (N_SECTION, C), 0.5, 3.0, ((0, 2),), jnp.float32),
        "leak_slope": jnp.clip(0.1 + 0.3 * jax.random.uniform(key_of[5], (N_SECTION, C), jnp.float32) ** levels(key_of[5], (N_SECTION, C), ((0, 2),), -0.2, 0.2), 0.1, 0.4),
        "depthwise": scatter_about(key_of[6], (SIDE * SIDE, C), (SIDE * SIDE) ** -0.5, 0.4375),
        "embed_weight": scatter_about(key_of[7], (C, EMB), C ** -0.5, 0.375),
        "class_centers": scatter_about(key_of[8], (CLASSES, EMB), 1.0, 6.0, ((0, 16),)),
        "labels": plant(jax.random.randint(key_of[9], (MICRO, FACES), 0, CLASSES), jax.random.fold_in(key_of[9], 1), 0, CLASSES - 1).astype(jnp.int32),
        "class_offsets": draw_class_offsets(jax.random.fold_in(key_of[11], 71), 0),
    }


margin_value = 0.4
scale_value = 64.0
tiny_value = 1e-06

def conv_apply(images, weights):
    image_count = images.shape[0]
    channels = images.shape[-1]
    image_grid = images.reshape(image_count, SIDE, SIDE, channels)
    padded = jnp.pad(image_grid, ((0, 0), (1, 1), (1, 1), (0, 0)))
    pieces = [padded[:, row_shift:row_shift + SIDE, col_shift:col_shift + SIDE, :] for row_shift in range(3) for col_shift in range(3)]
    columns = jnp.concatenate(pieces, axis=3).reshape(image_count * SIDE * SIDE, 9 * channels)
    result = jnp.dot(columns, weights, preferred_element_type=jnp.float32)
    return result.reshape(image_count, SIDE * SIDE, weights.shape[1])

def flip_weights(weights):
    channels = weights.shape[1]
    tap_blocks = weights.reshape(9, channels, channels)
    return jnp.swapaxes(tap_blocks[::-1], 1, 2).reshape(9 * channels, channels)

def smooth_active(pre_active, leak):
    return leak * pre_active + (1.0 - leak) * jax.nn.softplus(4.0 * pre_active) / 4.0

def smooth_slope(pre_active, leak):
    return leak + (1.0 - leak) * jax.nn.sigmoid(4.0 * pre_active)

def unit_forward(images, first_weight, second_weight, gain_row, bias_row, leak_row):
    hidden = conv_apply(images, first_weight)
    pre_active = hidden * gain_row + bias_row
    active = smooth_active(pre_active, leak_row).astype(jnp.bfloat16)
    output = (images.astype(jnp.float32) + conv_apply(active, second_weight)).astype(jnp.bfloat16)
    return (output, pre_active)

def unit_backward(grad_out, pre_active, first_flip, second_flip, gain_row, leak_row):
    grad_active = conv_apply(grad_out, second_flip)
    grad_hidden = (grad_active * smooth_slope(pre_active, leak_row) * gain_row).astype(jnp.bfloat16)
    return (grad_out.astype(jnp.float32) + conv_apply(grad_hidden, first_flip)).astype(jnp.bfloat16)

def unit_scale(values):
    squares = lax.optimization_barrier(jnp.mean(values * values, axis=-1, keepdims=True))
    factor = lax.rsqrt(squares + tiny_value) / math.sqrt(values.shape[-1])
    return (values * factor, squares, factor)

def reference(section_input, conv_one, conv_two, unit_gain, offset_bias, leak_slope, depthwise, embed_weight, class_centers, labels, class_offsets):
    row_count = MICRO * FACES
    current = section_input.reshape(row_count, SIDE * SIDE, C)
    pre_list = []
    for section_index in range(N_SECTION):
        current, pre_active = unit_forward(current, conv_one[section_index], conv_two[section_index], unit_gain[section_index], offset_bias[section_index], leak_slope[section_index])
        pre_list.append(pre_active)
    pooled = jnp.einsum('rpc,pc->rc', current.astype(jnp.float32), depthwise.astype(jnp.float32)).astype(jnp.bfloat16)
    embedded = jnp.dot(pooled, embed_weight, preferred_element_type=jnp.float32)
    normed, squares, factor = unit_scale(embedded)
    unit_half = normed.astype(jnp.bfloat16)
    flat_labels = labels.reshape(row_count)
    blocks = class_centers.reshape(N_SHARD, CLS_DEV, EMB)

    def one_block(running, inputs):
        center_block, class_base = inputs
        centres_unit = unit_scale(center_block.astype(jnp.float32))[0].astype(jnp.bfloat16)
        cosines = jnp.dot(unit_half, centres_unit.T, preferred_element_type=jnp.float32)
        class_ids = class_base + jnp.arange(CLS_DEV, dtype=jnp.int32)
        label_hits = flat_labels[:, None] == class_ids[None, :]
        logits = scale_value * (cosines - margin_value * label_hits.astype(jnp.float32))
        exp_logits = jnp.exp(logits)
        weighted = jnp.dot(exp_logits.astype(jnp.bfloat16), centres_unit, preferred_element_type=jnp.float32)
        chosen = jnp.dot(label_hits.astype(jnp.bfloat16), centres_unit, preferred_element_type=jnp.float32)
        return ((running[0] + weighted, running[1] + chosen, running[2] + lax.optimization_barrier(jnp.sum(exp_logits, axis=1))), None)
    start_sums = (jnp.zeros((row_count, EMB), jnp.float32), jnp.zeros((row_count, EMB), jnp.float32), jnp.zeros((row_count,), jnp.float32))
    sums_out = lax.scan(one_block, start_sums, (blocks, class_offsets.astype(jnp.int32)))[0]
    grad_unit = scale_value * (sums_out[0] / sums_out[2][:, None] - sums_out[1])
    inner = lax.optimization_barrier(jnp.sum(embedded * grad_unit, axis=-1, keepdims=True))
    grad_embed = factor * (grad_unit - embedded * inner / (EMB * (squares + tiny_value)))
    grad_pooled = jnp.dot(grad_embed.astype(jnp.bfloat16), embed_weight.T, preferred_element_type=jnp.float32)
    current_grad = (grad_pooled[:, None, :] * depthwise.astype(jnp.float32)[None, :, :]).astype(jnp.bfloat16)
    grad_list = [None] * N_SECTION
    for section_index in reversed(range(N_SECTION)):
        current_grad = unit_backward(current_grad, pre_list[section_index], flip_weights(conv_one[section_index]), flip_weights(conv_two[section_index]), unit_gain[section_index], leak_slope[section_index])
        grad_list[section_index] = current_grad
    return jnp.stack(grad_list).reshape(N_SECTION, MICRO, FACES, SIDE * SIDE, C)
```

```python
import functools
import math

import jax
import jax.numpy as jnp
from jax import lax
from jax.experimental import pallas as pl
from jax.experimental.pallas import tpu as pltpu
from jax.sharding import PartitionSpec as P

MESH = pl.DeviceIdType.MESH
STRIDE = 16
GUARD = 16
HALF_ROWS = 16
LANES = 128

margin_value = 0.4
scale_value = 64.0
tiny_value = 1e-06

f32 = jnp.float32
bf16 = jnp.bfloat16


def dot(left, right):
    return jnp.dot(left, right, preferred_element_type=f32)


def kernel(
    sections,
    shards,
    images,
    side,
    x_hbm,
    w1_hbm,
    w2_hbm,
    gain_hbm,
    bias_hbm,
    leak_hbm,
    depth_hbm,
    embed_hbm,
    centre_hbm,
    labels_hbm,
    offset_hbm,
    out_ref,
    xraw,
    xall,
    xin,
    xsend,
    gin,
    gout,
    oall,
    w1,
    w2,
    w1t,
    w2t,
    gain_ref,
    bias_ref,
    leak_ref,
    depth,
    embed,
    embed_t,
    raw,
    centres,
    centres_t,
    labels_ref,
    offset_ref,
    cols_a,
    cols_b,
    spread,
    padded,
    packed,
    dws,
    slope,
    emb,
    unit_src,
    unit_all,
    flat,
    wide,
    label_col,
    hits,
    picked,
    chosen_src,
    chosen_rcv,
    part_src,
    part_rcv,
    in_sem,
    xs_send,
    xs_recv,
    gs_send,
    gs_recv,
    peer_send,
    peer_recv,
):
    section = lax.axis_index("section")
    me = lax.axis_index("shard")
    first = section == 0
    last = section == sections - 1
    positions = side * side
    rows = side * STRIDE
    channels = w1.shape[1]
    folds = channels // LANES
    width = embed.shape[1]
    class_count = centres.shape[0]
    faces = images * shards
    body = pl.ds(STRIDE, rows)

    def bring(k, source, target):
        return pltpu.make_async_copy(source, target, in_sem.at[k])

    x_copy = bring(0, x_hbm, xraw)
    w1_copy = bring(1, w1_hbm.at[0], w1)
    w2_copy = bring(2, w2_hbm.at[0], w2)
    gain_copy = bring(3, gain_hbm, gain_ref)
    bias_copy = bring(4, bias_hbm, bias_ref)
    leak_copy = bring(5, leak_hbm, leak_ref)
    depth_copy = bring(6, depth_hbm, depth)
    embed_copy = bring(7, embed_hbm, embed)
    centre_copy = bring(8, centre_hbm, raw)
    labels_copy = bring(9, labels_hbm, labels_ref)
    offset_copy = bring(10, offset_hbm, offset_ref)

    @pl.when(first)
    def _():
        x_copy.start()

    @pl.when(last)
    def _():
        labels_copy.start()
        offset_copy.start()
        depth_copy.start()
        centre_copy.start()

    w1_copy.start()
    gain_copy.start()
    bias_copy.start()
    leak_copy.start()
    w2_copy.start()

    @pl.when(last)
    def _():
        embed_copy.start()

    barrier = pltpu.get_barrier_semaphore()

    @pl.when(section > 0)
    def _():
        pl.semaphore_signal(barrier, inc=1, device_id={"section": section - 1}, device_id_type=MESH)

    @pl.when(section < sections - 1)
    def _():
        pl.semaphore_signal(barrier, inc=1, device_id={"section": section + 1}, device_id_type=MESH)

    @pl.when(last)
    def _():
        @pl.loop(1, shards)
        def _(k):
            peer = lax.rem(me + k, shards)
            pl.semaphore_signal(barrier, inc=1, device_id={"shard": peer}, device_id_type=MESH)

    neighbours = jnp.where(first, 0, 1) + jnp.where(last, shards - 1, 1)

    def greet():
        with jax.named_scope("barrier"):
            pl.semaphore_wait(barrier, neighbours)

    for cols in (cols_a, cols_b):
        cols[pl.ds(0, STRIDE), :] = jnp.zeros((STRIDE, 3 * channels), bf16)
        cols[pl.ds(rows + STRIDE, STRIDE), :] = jnp.zeros((STRIDE, 3 * channels), bf16)
    for h in range(folds):
        padded[h, pl.ds(0, STRIDE), :] = jnp.zeros((STRIDE, LANES), f32)
        padded[h, pl.ds(rows + STRIDE, STRIDE), :] = jnp.zeros((STRIDE, LANES), f32)
        spread[h, pl.ds(0, GUARD), :] = jnp.zeros((GUARD, LANES), f32)
        tail = spread.shape[1] - GUARD - positions
        spread[h, pl.ds(GUARD + positions, tail), :] = jnp.zeros((tail, LANES), f32)

    column = lax.broadcasted_iota(jnp.int32, (STRIDE, LANES), 0)
    inside = {
        -1: (column >= 1) & (column < side),
        0: column < side,
        1: column < side - 1,
    }
    keep = (lax.broadcasted_iota(jnp.int32, (rows, LANES), 0) & (STRIDE - 1)) < side

    def lanes(h):
        return slice(h * LANES, (h + 1) * LANES)

    def spread_in(source):
        for h in range(folds):
            spread[h, pl.ds(GUARD, positions), :] = source[:, lanes(h)].astype(f32)

    def expand(store):
        for i in range(side):
            for d in (-1, 0, 1):
                for h in range(folds):
                    value = spread[h, pl.ds(GUARD + side * i + d, STRIDE), :]
                    store(i, d, h, jnp.where(inside[d], value, 0.0))

    def expand_cols():
        def store(i, d, h, value):
            target = pl.ds(channels * (d + 1) + LANES * h, LANES)
            cols_a[pl.ds(STRIDE * (i + 1), STRIDE), target] = value.astype(bf16)

        expand(store)

    def shift_cols():
        for h in range(folds):
            for d in (-1, 0, 1):
                target = pl.ds(channels * (d + 1) + LANES * h, LANES)
                cols_b[body, target] = padded[h, pl.ds(STRIDE + d, rows), :].astype(bf16)

    def centre_of(cols):
        return cols[body, pl.ds(channels, channels)].astype(f32)

    def compact(value):
        for i in range(side):
            for h in range(folds):
                packed[h, pl.ds(side * i, STRIDE), :] = value[STRIDE * i : STRIDE * (i + 1), lanes(h)]

    def packed_out(target):
        for h in range(folds):
            target[:, pl.ds(LANES * h, LANES)] = packed[h, pl.ds(0, positions), :].astype(bf16)

    cut = side // 2 * STRIDE
    depth3 = 3 * channels

    def conv(cols, weights):
        halves = []
        for start, count in ((0, cut), (cut, rows - cut)):
            total = dot(cols[pl.ds(start, count), :], weights[pl.ds(0, depth3), :])
            for d in (1, 2):
                total += dot(
                    cols[pl.ds(start + STRIDE * d, count), :], weights[pl.ds(depth3 * d, depth3), :]
                )
            halves.append(total)
        return jnp.concatenate(halves, axis=0)

    def flip():
        with jax.named_scope("flip"):

            @pl.loop(0, 9)
            def _(t):
                there = pl.ds(pl.multiple_of(t * channels, channels), channels)
                here = pl.ds(pl.multiple_of((8 - t) * channels, channels), channels)
                w2t[there, :] = w2[here, :].T
                w1t[there, :] = w1[here, :].T

    sources = (unit_src, chosen_src, part_src)
    targets = (unit_all, chosen_rcv, part_rcv)

    def peer_copy(kind, m, to):
        source = sources[kind].at[m]
        return pltpu.make_async_remote_copy(
            src_ref=source if kind == 0 else source.at[to],
            dst_ref=targets[kind].at[m, me],
            send_sem=peer_send.at[kind, m],
            recv_sem=peer_recv.at[kind, m],
            device_id={"shard": to},
            device_id_type=MESH,
        )

    def send_peers(kind, m):
        @pl.loop(1, shards)
        def _(k):
            peer_copy(kind, m, lax.rem(me + k, shards)).start()

    def peers_all(kind, m):
        others = targets[kind].at[m, pl.ds(0, shards - 1)]
        return pltpu.make_async_remote_copy(
            src_ref=others,
            dst_ref=others,
            send_sem=peer_send.at[kind, m],
            recv_sem=peer_recv.at[kind, m],
            device_id={"shard": lax.rem(me + 1, shards)},
            device_id_type=MESH,
        )

    def recv_peers(kind, m):
        peers_all(kind, m).wait_recv()

    def drain_peers(kind, m):
        peers_all(kind, m).wait_send()

    @pl.when(last)
    def _():
        labels_copy.wait()
        offset_copy.wait()
        micro = labels_ref.shape[0]
        local = images // micro
        row = lax.broadcasted_iota(jnp.int32, (shards, labels_ref.shape[1]), 0)
        lane = lax.broadcasted_iota(jnp.int32, (shards, labels_ref.shape[1]), 1)
        for m in range(micro):
            values = labels_ref[pl.ds(m, 1), :].astype(f32)
            for f in range(local):
                mine = jnp.where(lane == row * local + f, values, 0.0)
                label_col[pl.ds((m * local + f) * shards, shards), :] = jnp.sum(mine, axis=1, keepdims=True)
        ids = lax.broadcasted_iota(jnp.int32, (faces, class_count), 1)
        wanted = label_col[...].astype(jnp.int32) - offset_ref[0]
        hits[...] = jnp.where(wanted == ids, 1.0, 0.0).astype(bf16)

        depth_copy.wait()
        spread_in(depth)

        def store(i, d, h, value):
            dws[d + 1, pl.ds(STRIDE * i, STRIDE), pl.ds(LANES * h, LANES)] = value

        expand(store)
        with jax.named_scope("centre_wait"):
            centre_copy.wait()
        block = LANES

        @pl.loop(0, class_count // block)
        def _(b):
            part = pl.ds(pl.multiple_of(b * block, block), block)
            values = raw[part, :].astype(f32)
            square = jnp.mean(values * values, axis=-1, keepdims=True)
            factor = lax.rsqrt(square + tiny_value) / math.sqrt(width)
            normed = (values * factor).astype(bf16)
            centres[part, :] = normed
            centres_t[:, part] = normed.T

        picked[...] = dot(hits[...], centres[...])
        for m in range(images):
            for n in range(shards):
                chosen_src[m, n] = picked[pl.ds(m * shards + n, 1), :]
            chosen_rcv[m, me] = chosen_src[m, me]
        greet()

        @pl.loop(0, images)
        def _(m):
            send_peers(1, m)

        embed_copy.wait()
        embed_t[...] = embed[...].T

    @pl.when(first)
    def _():
        x_copy.wait()
        xall[...] = xraw[...].astype(f32)

    gain_copy.wait()
    bias_copy.wait()
    leak_copy.wait()
    gain = gain_ref[...]
    bias = bias_ref[...]
    leak = leak_ref[...]
    half = (0.5 * (1.0 - leak)) * gain
    base = leak * gain + half
    quarter = 0.25 * (1.0 - leak)
    with jax.named_scope("w_wait"):
        w1_copy.wait()
        w2_copy.wait()

    @pl.when(last)
    def _():
        flip()

    def x_send(m, step=1):
        return pltpu.make_async_remote_copy(
            src_ref=xsend.at[m],
            dst_ref=xin.at[m],
            send_sem=xs_send.at[m],
            recv_sem=xs_recv.at[m],
            device_id={"section": section + step},
            device_id_type=MESH,
        )

    def g_send(m, step=-1):
        return pltpu.make_async_remote_copy(
            src_ref=gout.at[m],
            dst_ref=gin.at[m],
            send_sem=gs_send.at[m],
            recv_sem=gs_recv.at[m],
            device_id={"section": section + step},
            device_id_type=MESH,
        )

    def forward(m):
        @pl.when(first)
        def _():
            for h in range(folds):
                spread[h, pl.ds(GUARD, positions), :] = xall[
                    pl.ds(h * images + m, positions, stride=folds * images), :
                ]

        @pl.when(section > 0)
        def _():
            with jax.named_scope("x_wait"):
                x_send(m, -1).wait_recv()
            spread_in(xin.at[m])

        expand_cols()
        z = conv(cols_a, w1) * gain + bias
        turn = jnp.tanh(z + z)
        share = base + half * turn
        active = jnp.maximum(z, leak * z) - quarter * jnp.log(0.5 + 0.5 * jnp.abs(turn))
        for h in range(folds):
            slope[m, :, lanes(h)] = jnp.where(keep, share[:, lanes(h)], 0.0)
            padded[h, body, :] = jnp.where(keep, active[:, lanes(h)], 0.0)
        shift_cols()
        y = centre_of(cols_a) + conv(cols_b, w2)

        @pl.when(section < sections - 1)
        def _():
            compact(y)
            packed_out(xsend.at[m])

            @pl.when(m == 0)
            def _():
                greet()

            x_send(m).start()

        @pl.when(last)
        def _():
            pooled = jnp.sum(y.astype(bf16).astype(f32) * dws[1], axis=0, keepdims=True)
            pooled = jnp.broadcast_to(pooled, (HALF_ROWS, channels)).astype(bf16)
            embedded = dot(pooled, embed[...])[:1]
            square = jnp.mean(embedded * embedded, axis=-1, keepdims=True)
            factor = lax.rsqrt(square + tiny_value) / math.sqrt(width)
            normed = (embedded * factor).astype(bf16).astype(f32)
            emb[m] = embedded
            unit_src[m] = normed
            unit_all[m, me] = normed
            send_peers(0, m)

    def partial(m):
        with jax.named_scope("unit_wait"):
            recv_peers(0, m)
        for n in range(shards):
            flat[pl.ds(n, 1), :] = unit_all[m, n]
        cosines = dot(flat[...].astype(bf16), centres_t[...])
        mine = pl.ds(pl.multiple_of(m * shards, shards), shards)
        logits = scale_value * (cosines - margin_value * hits[mine, :].astype(f32))
        grown = jnp.exp(logits)
        wide[:, pl.ds(0, width)] = dot(grown.astype(bf16), centres[...])
        wide[:, pl.ds(width, LANES)] = jnp.broadcast_to(
            jnp.sum(grown, axis=1, keepdims=True), (shards, LANES)
        )
        for n in range(shards):
            part_src[m, n] = wide[pl.ds(n, 1), :]
        part_rcv[m, me] = part_src[m, me]
        send_peers(2, m)

    def backward(m):
        @pl.when(last)
        def _():
            with jax.named_scope("chosen_wait"):
                recv_peers(1, m)
            chosen = jnp.sum(chosen_rcv[m], axis=0)
            with jax.named_scope("part_wait"):
                recv_peers(2, m)
            sums = jnp.sum(part_rcv[m], axis=0)
            grad_unit = scale_value * (sums[:, :width] / sums[:, width : width + 1] - chosen)
            embedded = emb[m]
            square = jnp.mean(embedded * embedded, axis=-1, keepdims=True)
            factor = lax.rsqrt(square + tiny_value) / math.sqrt(width)
            inner = jnp.sum(embedded * grad_unit, axis=-1, keepdims=True)
            grad_embed = factor * (
                grad_unit - embedded * inner / (width * (square + tiny_value))
            )
            grad_embed = jnp.broadcast_to(grad_embed, (HALF_ROWS, width)).astype(bf16)
            gpool = dot(grad_embed, embed_t[...])[:1]
            for d in range(3):
                cols_a[body, pl.ds(channels * d, channels)] = (gpool * dws[d]).astype(bf16)

        @pl.when(section < sections - 1)
        def _():
            with jax.named_scope("g_wait"):
                g_send(m, 1).wait_recv()
            spread_in(gin.at[m])
            expand_cols()

        hidden = conv(cols_a, w2t) * slope[m]
        for h in range(folds):
            padded[h, body, :] = hidden[:, lanes(h)]
        shift_cols()
        compact(centre_of(cols_a) + conv(cols_b, w1t))

        @pl.when(section > 0)
        def _():
            packed_out(gout.at[m])
            g_send(m).start()

        for h in range(folds):
            oall[pl.ds(h * images + m, positions, stride=folds * images), :] = packed[
                h, pl.ds(0, positions), :
            ]

    def drain():
        @pl.loop(0, images)
        def _(m):
            @pl.when(section < sections - 1)
            def _():
                x_send(m).wait_send()

            @pl.when(section > 0)
            def _():
                g_send(m).wait_send()

        @pl.when(last)
        def _():
            @pl.loop(0, images)
            def _(m):
                for kind in range(3):
                    drain_peers(kind, m)

    lag = 4

    @pl.loop(0, images + lag)
    def _(t):
        @pl.when(t < images)
        def _():
            with jax.named_scope("forward"):
                forward(t)

        @pl.when((section < sections - 1) & (t == images - 1))
        def _():
            flip()

        @pl.when(last & (t >= 2) & (t < images + 2))
        def _():
            with jax.named_scope("partial"):
                partial(t - 2)

        @pl.when(t >= lag)
        def _():
            with jax.named_scope("backward"):
                backward(t - lag)

    with jax.named_scope("drain"):
        out_ref[...] = oall[...].astype(bf16)
        drain()


def emit(source, target, sem):
    copy = pltpu.make_async_copy(source, target, sem)
    copy.start()
    copy.wait()


def on_device(
    section_input,
    conv_one,
    conv_two,
    unit_gain,
    offset_bias,
    leak_slope,
    depthwise,
    embed_weight,
    class_centers,
    labels,
    class_offsets,
):
    sections = lax.axis_size("section")
    shards = lax.axis_size("shard")
    micro, local, positions, channels = section_input.shape
    side = math.isqrt(positions)
    images = micro * local
    rows = side * STRIDE
    folds = channels // LANES
    width = embed_weight.shape[1]
    classes = class_centers.shape[0]
    faces = shards * images
    hbm = pl.BlockSpec(memory_space=pltpu.HBM)
    vmem = pl.BlockSpec(memory_space=pltpu.VMEM)
    dma = pltpu.SemaphoreType.DMA
    vm = pltpu.VMEM
    lined = (positions * folds * images, LANES)
    maps = vm((images, positions, channels), bf16)
    weights = vm(conv_one.shape[1:], bf16)
    columns = vm((rows + 2 * STRIDE, 3 * channels), bf16)
    row = vm((1, channels), f32)
    result = pl.pallas_call(
        functools.partial(kernel, sections, shards, images, side),
        out_shape=vm(lined, bf16),
        in_specs=[hbm] * 11,
        out_specs=vmem,
        scratch_shapes=[
            vm(lined, bf16),
            vm(lined, f32),
            maps,
            maps,
            maps,
            maps,
            vm(lined, f32),
            weights,
            weights,
            weights,
            weights,
            row,
            row,
            row,
            vm((positions, channels), bf16),
            vm(embed_weight.shape, bf16),
            vm((width, channels), bf16),
            vm((classes, width), bf16),
            vm((classes, width), bf16),
            vm((width, classes), bf16),
            vm(labels.shape, jnp.int32),
            pltpu.SMEM(class_offsets.shape, jnp.int32),
            columns,
            columns,
            vm((folds, GUARD + -(-positions // 8) * 8 + 8, LANES), f32),
            vm((folds, rows + 2 * STRIDE, LANES), f32),
            vm((folds, -(-(positions + STRIDE - side) // 8) * 8, LANES), f32),
            vm((3, rows, channels), f32),
            vm((images, rows, channels), f32),
            vm((images, 1, width), f32),
            vm((images, 1, width), f32),
            vm((images, shards, 1, width), f32),
            vm((shards, width), f32),
            vm((shards, width + LANES), f32),
            vm((faces, 1), f32),
            vm((faces, classes), bf16),
            vm((faces, width), f32),
            vm((images, shards, 1, width), f32),
            vm((images, shards, 1, width), f32),
            vm((images, shards, 1, width + LANES), f32),
            vm((images, shards, 1, width + LANES), f32),
            dma((11,)),
            dma((images,)),
            dma((images,)),
            dma((images,)),
            dma((images,)),
            dma((3, images)),
            dma((3, images)),
        ],
        compiler_params=pltpu.CompilerParams(
            collective_id=0, has_side_effects=True, vmem_limit_bytes=60000 * 1024
        ),
        name="window",
    )(
        section_input.reshape(images, positions, folds, LANES).transpose(1, 2, 0, 3).reshape(lined),
        conv_one,
        conv_two,
        unit_gain,
        offset_bias,
        leak_slope,
        depthwise,
        embed_weight,
        class_centers,
        labels,
        class_offsets,
    )
    result = pl.pallas_call(
        emit,
        out_shape=jax.ShapeDtypeStruct(lined, bf16),
        in_specs=[vmem],
        out_specs=hbm,
        scratch_shapes=[dma],
        name="emit",
    )(pltpu.with_memory_space_constraint(result, pltpu.VMEM))
    result = result.reshape(positions, folds, images, LANES).transpose(2, 0, 1, 3)
    return result.reshape(1, micro, local, positions, channels)


def solution(mesh):
    placed = (
        P(None, "shard", None, None),
        P("section", None, None),
        P("section", None, None),
        P("section", None),
        P("section", None),
        P("section", None),
        P(),
        P(),
        P("shard", None),
        P(),
        P("shard"),
    )
    return jax.shard_map(
        on_device,
        mesh=mesh,
        in_specs=placed,
        out_specs=P("section", None, "shard", None, None),
        check_vma=False,
    )
```

```python
import functools
import math

import jax
import jax.numpy as jnp
from jax import lax
from jax.experimental import pallas as pl
from jax.experimental.pallas import tpu as pltpu
from jax.sharding import PartitionSpec as P

MESH = pl.DeviceIdType.MESH
STRIDE = 16
GUARD = 16
HALF_ROWS = 16
LANES = 128

margin_value = 0.4
scale_value = 64.0
tiny_value = 1e-06
lowest = -3e38

f32 = jnp.float32
bf16 = jnp.bfloat16


def dot(left, right):
    return jnp.dot(left, right, preferred_element_type=f32)


def kernel(
    sections,
    shards,
    images,
    side,
    x_hbm,
    w1_hbm,
    w2_hbm,
    gain_hbm,
    bias_hbm,
    leak_hbm,
    depth_hbm,
    embed_hbm,
    centre_hbm,
    labels_hbm,
    offset_hbm,
    out_ref,
    xraw,
    xall,
    xin,
    xsend,
    gin,
    gout,
    oall,
    w1,
    w2,
    w1t,
    w2t,
    gain_ref,
    bias_ref,
    leak_ref,
    depth,
    embed,
    embed_t,
    raw,
    centres,
    centres_t,
    labels_ref,
    offset_ref,
    cols_a,
    cols_b,
    spread,
    padded,
    packed,
    dws,
    slope,
    emb,
    scales,
    unit_src,
    unit_all,
    flat,
    wide,
    label_col,
    hits,
    picked,
    chosen_src,
    chosen_rcv,
    part_src,
    part_rcv,
    in_sem,
    xs_send,
    xs_recv,
    gs_send,
    gs_recv,
    peer_send,
    peer_recv,
):
    section = lax.axis_index("section")
    me = lax.axis_index("shard")
    first = section == 0
    last = section == sections - 1
    positions = side * side
    rows = side * STRIDE
    channels = w1.shape[1]
    folds = channels // LANES
    width = embed.shape[1]
    class_count = centres.shape[0]
    faces = images * shards
    body = pl.ds(STRIDE, rows)

    def bring(k, source, target):
        return pltpu.make_async_copy(source, target, in_sem.at[k])

    x_copy = bring(0, x_hbm, xraw)
    w1_copy = bring(1, w1_hbm.at[0], w1)
    w2_copy = bring(2, w2_hbm.at[0], w2)
    gain_copy = bring(3, gain_hbm, gain_ref)
    bias_copy = bring(4, bias_hbm, bias_ref)
    leak_copy = bring(5, leak_hbm, leak_ref)
    depth_copy = bring(6, depth_hbm, depth)
    embed_copy = bring(7, embed_hbm, embed)
    centre_copy = bring(8, centre_hbm, raw)
    labels_copy = bring(9, labels_hbm, labels_ref)
    offset_copy = bring(10, offset_hbm, offset_ref)

    @pl.when(first)
    def _():
        x_copy.start()

    @pl.when(last)
    def _():
        labels_copy.start()
        offset_copy.start()
        depth_copy.start()
        centre_copy.start()

    w1_copy.start()
    gain_copy.start()
    bias_copy.start()
    leak_copy.start()
    w2_copy.start()

    @pl.when(last)
    def _():
        embed_copy.start()

    barrier = pltpu.get_barrier_semaphore()

    @pl.when(section > 0)
    def _():
        pl.semaphore_signal(barrier, inc=1, device_id={"section": section - 1}, device_id_type=MESH)

    @pl.when(section < sections - 1)
    def _():
        pl.semaphore_signal(barrier, inc=1, device_id={"section": section + 1}, device_id_type=MESH)

    @pl.when(last)
    def _():
        for k in range(1, shards):
            peer = lax.rem(me + k, shards)
            pl.semaphore_signal(barrier, inc=1, device_id={"shard": peer}, device_id_type=MESH)

    neighbours = jnp.where(first, 0, 1) + jnp.where(last, shards - 1, 1)

    def greet():
        with jax.named_scope("barrier"):
            pl.semaphore_wait(barrier, neighbours)

    for cols in (cols_a, cols_b):
        cols[pl.ds(0, STRIDE), :] = jnp.zeros((STRIDE, 3 * channels), bf16)
        cols[pl.ds(rows + STRIDE, STRIDE), :] = jnp.zeros((STRIDE, 3 * channels), bf16)
    for h in range(folds):
        padded[h, pl.ds(0, STRIDE), :] = jnp.zeros((STRIDE, LANES), f32)
        padded[h, pl.ds(rows + STRIDE, STRIDE), :] = jnp.zeros((STRIDE, LANES), f32)
        spread[h, pl.ds(0, GUARD), :] = jnp.zeros((GUARD, LANES), f32)
        tail = spread.shape[1] - GUARD - positions
        spread[h, pl.ds(GUARD + positions, tail), :] = jnp.zeros((tail, LANES), f32)
        packed[h, pl.ds(packed.shape[1] - 8, 8), :] = jnp.zeros((8, LANES), f32)

    column = lax.broadcasted_iota(jnp.int32, (STRIDE, LANES), 0)
    inside = {
        -1: (column >= 1) & (column < side),
        0: column < side,
        1: column < side - 1,
    }
    keep = (lax.broadcasted_iota(jnp.int32, (rows, LANES), 0) & (STRIDE - 1)) < side

    def lanes(h):
        return slice(h * LANES, (h + 1) * LANES)

    def spread_in(source):
        for h in range(folds):
            spread[h, pl.ds(GUARD, positions), :] = source[pl.ds(0, positions), lanes(h)].astype(f32)

    def expand(store):
        for i in range(side):
            for d in (-1, 0, 1):
                for h in range(folds):
                    value = spread[h, pl.ds(GUARD + side * i + d, STRIDE), :]
                    store(i, d, h, jnp.where(inside[d], value, 0.0))

    def expand_cols():
        def store(i, d, h, value):
            target = pl.ds(channels * (d + 1) + LANES * h, LANES)
            cols_a[pl.ds(STRIDE * (i + 1), STRIDE), target] = value.astype(bf16)

        expand(store)

    def shift_cols(start, count):
        for h in range(folds):
            for d in (-1, 0, 1):
                target = pl.ds(channels * (d + 1) + LANES * h, LANES)
                source = padded[h, pl.ds(STRIDE + start + d, count), :]
                cols_b[pl.ds(STRIDE + start, count), target] = source.astype(bf16)

    def centre_of(start, count):
        return cols_a[pl.ds(STRIDE + start, count), pl.ds(channels, channels)].astype(f32)

    depth3 = 3 * channels

    def chain(cols, weights, start, count, taps):
        total = None
        for d in range(3):
            low, high = max(taps[0] - 3 * d, 0), min(taps[1] - 3 * d, 3)
            if low < high:
                left = cols[pl.ds(start + STRIDE * d, count), pl.ds(channels * low, channels * (high - low))]
                right = weights[pl.ds(depth3 * d + channels * low, channels * (high - low)), :]
                term = dot(left, right)
                total = term if total is None else total + term
        return total

    def conv(cols, weights, cut):
        for start, count, middle in ((0, cut, 5), (cut, rows - cut, 4)):
            one = chain(cols, weights, start, count, (0, middle))
            two = chain(cols, weights, start, count, (middle, 9))
            yield start, count, one + jnp.maximum(two, lowest)

    half_rows = side // 2 * STRIDE
    send_cut = side // 2 * side // 8 * 8
    parts = ((0, send_cut), (send_cut, packed.shape[1] - send_cut))

    def compact(start, value):
        for i in range(value.shape[0] // STRIDE):
            for h in range(folds):
                piece = value[STRIDE * i : STRIDE * (i + 1), lanes(h)]
                packed[h, pl.ds(side * (start // STRIDE + i), STRIDE), :] = piece

    def collect(m, start, value):
        for i in range(value.shape[0] // STRIDE):
            for h in range(folds):
                piece = value[STRIDE * i : STRIDE * (i + 1), lanes(h)]
                where = (side * (start // STRIDE + i) * folds + h) * images + m
                oall[pl.ds(where, STRIDE, stride=folds * images), :] = piece

    def packed_out(target, part):
        low, count = parts[part]
        for h in range(folds):
            target[pl.ds(low, count), pl.ds(LANES * h, LANES)] = packed[h, pl.ds(low, count), :].astype(bf16)

    def flip():
        with jax.named_scope("flip"):

            @pl.loop(0, 9)
            def _(t):
                there = pl.ds(pl.multiple_of(t * channels, channels), channels)
                here = pl.ds(pl.multiple_of((8 - t) * channels, channels), channels)
                w2t[there, :] = w2[here, :].T
                w1t[there, :] = w1[here, :].T

    sources = (unit_src, chosen_src, part_src)
    targets = (unit_all, chosen_rcv, part_rcv)

    def peer_copy(kind, m, to):
        source = sources[kind].at[m]
        return pltpu.make_async_remote_copy(
            src_ref=source if kind == 0 else source.at[to],
            dst_ref=targets[kind].at[m, me],
            send_sem=peer_send.at[kind, m],
            recv_sem=peer_recv.at[kind, m],
            device_id={"shard": to},
            device_id_type=MESH,
        )

    order = [k for k in range(3 * shards // 4, shards)] + [k for k in range(1, 3 * shards // 4)]

    def send_peers(kind, m):
        for k in order:
            peer_copy(kind, m, lax.rem(me + k, shards)).start()

    def peers_all(kind, m):
        others = targets[kind].at[m, pl.ds(0, shards - 1)]
        return pltpu.make_async_remote_copy(
            src_ref=others,
            dst_ref=others,
            send_sem=peer_send.at[kind, m],
            recv_sem=peer_recv.at[kind, m],
            device_id={"shard": lax.rem(me + 1, shards)},
            device_id_type=MESH,
        )

    def recv_peers(kind, m):
        peers_all(kind, m).wait_recv()

    def drain_peers(kind, m):
        peers_all(kind, m).wait_send()

    def x_send(m, part, step=1):
        window = pl.ds(*parts[part])
        return pltpu.make_async_remote_copy(
            src_ref=xsend.at[m, window],
            dst_ref=xin.at[m, window],
            send_sem=xs_send.at[m, part],
            recv_sem=xs_recv.at[m, part],
            device_id={"section": section + step},
            device_id_type=MESH,
        )

    def g_send(m, part, step=-1):
        window = pl.ds(*parts[part])
        return pltpu.make_async_remote_copy(
            src_ref=gout.at[m, window],
            dst_ref=gin.at[m, window],
            send_sem=gs_send.at[m, part],
            recv_sem=gs_recv.at[m, part],
            device_id={"section": section + step},
            device_id_type=MESH,
        )

    def receive(copy, m, step, landing):
        for part in range(2):
            copy(m, part, step).wait_recv()
        spread_in(landing.at[m])

    def forward(m, finish, between=None):
        gain = gain_ref[...]
        bias = bias_ref[...]
        leak = leak_ref[...]
        half = (0.5 * (1.0 - leak)) * gain
        base = leak * gain + half
        quarter = 0.25 * (1.0 - leak)
        for start, count, total in conv(cols_a, w1, half_rows + STRIDE):
            z = total * gain + bias
            turn = jnp.tanh(z + z)
            share = base + half * turn
            active = jnp.maximum(z, leak * z) - quarter * jnp.log(0.5 + 0.5 * jnp.abs(turn))
            mask = keep[:count]
            for h in range(folds):
                slope[m, pl.ds(start, count), lanes(h)] = jnp.where(mask, share[:, lanes(h)], 0.0)
                padded[h, pl.ds(STRIDE + start, count), :] = jnp.where(mask, active[:, lanes(h)], 0.0)
            shift_cols(start, count)
        if between is not None:
            between()
        for part, (start, count, total) in enumerate(conv(cols_b, w2, half_rows)):
            finish(part, start, centre_of(start, count) + total)

    def backward(m, finish):
        for start, count, total in conv(cols_a, w2t, half_rows + STRIDE):
            hidden = total * slope[m, pl.ds(start, count), :]
            for h in range(folds):
                padded[h, pl.ds(STRIDE + start, count), :] = hidden[:, lanes(h)]
            shift_cols(start, count)
        for part, (start, count, total) in enumerate(conv(cols_b, w1t, half_rows)):
            finish(part, start, centre_of(start, count) + total)

    def small_waits():
        gain_copy.wait()
        bias_copy.wait()
        leak_copy.wait()

    @pl.when(section < sections - 1)
    def _():
        @pl.when(first)
        def _():
            with jax.named_scope("w_wait"):
                x_copy.wait()
            xall[...] = xraw[...].astype(f32)

        small_waits()
        with jax.named_scope("w_wait"):
            w1_copy.wait()

        def run(m, peeled):
            @pl.when(first)
            def _():
                for h in range(folds):
                    spread[h, pl.ds(GUARD, positions), :] = xall[
                        pl.ds(h * images + m, positions, stride=folds * images), :
                    ]

            @pl.when(section > 0)
            def _():
                receive(x_send, m, -1, xin)

            expand_cols()

            def finish(part, start, value):
                compact(start, value)
                packed_out(xsend.at[m], part)
                if peeled and part == 0:
                    greet()
                x_send(m, part).start()

            forward(m, finish, w2_copy.wait if peeled else None)

        with jax.named_scope("forward"):
            run(0, True)

        @pl.loop(1, images)
        def _(m):
            with jax.named_scope("forward"):
                run(m, False)

        flip()

        @pl.loop(0, images)
        def _(m):
            with jax.named_scope("g_wait"):
                for part in range(2):
                    g_send(m, part, 1).wait_recv()
            with jax.named_scope("backward"):
                spread_in(gin.at[m])
                expand_cols()

                def finish(part, start, value):
                    compact(start, value)
                    collect(m, start, value)

                backward(m, finish)

                @pl.when(section > 0)
                def _():
                    for part in range(2):
                        packed_out(gout.at[m], part)
                        g_send(m, part).start()

    @pl.when(last)
    def _():
        labels_copy.wait()
        offset_copy.wait()
        micro = labels_ref.shape[0]
        local = images // micro
        row = lax.broadcasted_iota(jnp.int32, (shards, labels_ref.shape[1]), 0)
        lane = lax.broadcasted_iota(jnp.int32, (shards, labels_ref.shape[1]), 1)
        for m in range(micro):
            values = labels_ref[pl.ds(m, 1), :].astype(f32)
            for f in range(local):
                mine = jnp.where(lane == row * local + f, values, 0.0)
                label_col[pl.ds((m * local + f) * shards, shards), :] = jnp.sum(mine, axis=1, keepdims=True)
        ids = lax.broadcasted_iota(jnp.int32, (faces, class_count), 1)
        wanted = label_col[...].astype(jnp.int32) - offset_ref[0]
        hits[...] = jnp.where(wanted == ids, 1.0, 0.0).astype(bf16)

        depth_copy.wait()
        spread_in(depth)

        def store(i, d, h, value):
            dws[d + 1, pl.ds(STRIDE * i, STRIDE), pl.ds(LANES * h, LANES)] = value

        expand(store)
        with jax.named_scope("centre_wait"):
            centre_copy.wait()
        block = LANES

        @pl.loop(0, class_count // block)
        def _(b):
            part = pl.ds(pl.multiple_of(b * block, block), block)
            values = raw[part, :].astype(f32)
            square = jnp.mean(values * values, axis=-1, keepdims=True)
            factor = lax.rsqrt(square + tiny_value) / math.sqrt(width)
            normed = (values * factor).astype(bf16)
            centres[part, :] = normed
            centres_t[:, part] = normed.T

        picked[...] = dot(hits[...], centres[...])
        for m in range(images):
            for n in range(shards):
                chosen_src[m, n] = picked[pl.ds(m * shards + n, 1), :]
            chosen_rcv[m, me] = chosen_src[m, me]
        embed_copy.wait()
        embed_t[...] = embed[...].T
        small_waits()
        with jax.named_scope("w_wait"):
            w1_copy.wait()
            w2_copy.wait()
        flip()
        greet()

        def last_forward(m):
            with jax.named_scope("x_wait"):
                receive(x_send, m, -1, xin)
            expand_cols()
            sums = []

            def finish(part, start, value):
                weighted = value.astype(bf16).astype(f32) * dws[1, pl.ds(start, value.shape[0]), :]
                sums.append(jnp.sum(weighted, axis=0, keepdims=True))

            forward(m, finish)
            pooled = jnp.broadcast_to(sums[0] + sums[1], (HALF_ROWS, channels)).astype(bf16)
            embedded = dot(pooled, embed[...])[:1]
            square = jnp.mean(embedded * embedded, axis=-1, keepdims=True)
            factor = lax.rsqrt(square + tiny_value) / math.sqrt(width)
            normed = (embedded * factor).astype(bf16).astype(f32)
            emb[m] = embedded
            unit_src[m] = normed
            unit_all[m, me] = normed
            send_peers(0, m)
            scales[m, pl.ds(0, 1), :] = jnp.broadcast_to(factor, (1, LANES))
            scales[m, pl.ds(1, 1), :] = jnp.broadcast_to(1.0 / (width * (square + tiny_value)), (1, LANES))
            send_peers(1, m)

        def partial(m):
            with jax.named_scope("unit_wait"):
                recv_peers(0, m)
            for n in range(shards):
                flat[pl.ds(n, 1), :] = unit_all[m, n]
            cosines = dot(flat[...].astype(bf16), centres_t[...])
            mine = pl.ds(pl.multiple_of(m * shards, shards), shards)
            logits = scale_value * (cosines - margin_value * hits[mine, :].astype(f32))
            grown = jnp.exp(logits)
            wide[:, pl.ds(0, width)] = dot(grown.astype(bf16), centres[...])
            wide[:, pl.ds(width, LANES)] = jnp.broadcast_to(
                jnp.sum(grown, axis=1, keepdims=True), (shards, LANES)
            )
            for n in range(shards):
                part_src[m, n] = wide[pl.ds(n, 1), :]
            part_rcv[m, me] = part_src[m, me]
            send_peers(2, m)

        def last_backward(m):
            with jax.named_scope("chosen_wait"):
                recv_peers(1, m)
            chosen = jnp.sum(chosen_rcv[m], axis=0)
            with jax.named_scope("part_wait"):
                recv_peers(2, m)
            sums = jnp.sum(part_rcv[m], axis=0)
            grad_unit = scale_value * (sums[:, :width] / sums[:, width : width + 1] - chosen)
            embedded = emb[m]
            factor = scales[m, 0:1, 0:1]
            shrink = scales[m, 1:2, 0:1]
            inner = jnp.sum(embedded * grad_unit, axis=-1, keepdims=True)
            grad_embed = factor * (grad_unit - embedded * (inner * shrink))
            grad_embed = jnp.broadcast_to(grad_embed, (HALF_ROWS, width)).astype(bf16)
            gpool = dot(grad_embed, embed_t[...])[:1]
            for d in range(3):
                cols_a[body, pl.ds(channels * d, channels)] = (gpool * dws[d]).astype(bf16)

            def finish(part, start, value):
                compact(start, value)
                packed_out(gout.at[m], part)
                g_send(m, part).start()
                collect(m, start, value)

            backward(m, finish)

        lag = 4

        @pl.loop(0, images + lag)
        def _(t):
            @pl.when(t < images)
            def _():
                with jax.named_scope("forward"):
                    last_forward(t)

            @pl.when((t >= 2) & (t < images + 2))
            def _():
                with jax.named_scope("partial"):
                    partial(t - 2)

            @pl.when(t >= lag)
            def _():
                with jax.named_scope("backward"):
                    last_backward(t - lag)

    with jax.named_scope("drain"):
        out_ref[...] = oall[pl.ds(0, positions * folds * images), :].astype(bf16)

        @pl.loop(0, images)
        def _(m):
            for part in range(2):

                @pl.when(section < sections - 1)
                def _():
                    x_send(m, part).wait_send()

                @pl.when(section > 0)
                def _():
                    g_send(m, part).wait_send()

        @pl.when(last)
        def _():
            @pl.loop(0, images)
            def _(m):
                for kind in range(3):
                    drain_peers(kind, m)


def emit(source, target, sem):
    copy = pltpu.make_async_copy(source, target, sem)
    copy.start()
    copy.wait()


def on_device(
    section_input,
    conv_one,
    conv_two,
    unit_gain,
    offset_bias,
    leak_slope,
    depthwise,
    embed_weight,
    class_centers,
    labels,
    class_offsets,
):
    sections = lax.axis_size("section")
    shards = lax.axis_size("shard")
    micro, local, positions, channels = section_input.shape
    side = math.isqrt(positions)
    images = micro * local
    rows = side * STRIDE
    folds = channels // LANES
    width = embed_weight.shape[1]
    classes = class_centers.shape[0]
    faces = shards * images
    hbm = pl.BlockSpec(memory_space=pltpu.HBM)
    vmem = pl.BlockSpec(memory_space=pltpu.VMEM)
    dma = pltpu.SemaphoreType.DMA
    vm = pltpu.VMEM
    lined = (positions * folds * images, LANES)
    taller = -(-(positions + STRIDE - side) // 8) * 8
    maps = vm((images, taller, channels), bf16)
    weights = vm(conv_one.shape[1:], bf16)
    columns = vm((rows + 2 * STRIDE, 3 * channels), bf16)
    row = vm((1, channels), f32)
    result = pl.pallas_call(
        functools.partial(kernel, sections, shards, images, side),
        out_shape=vm(lined, bf16),
        in_specs=[hbm] * 11,
        out_specs=vmem,
        scratch_shapes=[
            vm(lined, bf16),
            vm(lined, f32),
            maps,
            maps,
            maps,
            maps,
            vm(((positions + STRIDE - side) * folds * images, LANES), f32),
            weights,
            weights,
            weights,
            weights,
            row,
            row,
            row,
            vm((positions, channels), bf16),
            vm(embed_weight.shape, bf16),
            vm((width, channels), bf16),
            vm((classes, width), bf16),
            vm((classes, width), bf16),
            vm((width, classes), bf16),
            vm(labels.shape, jnp.int32),
            pltpu.SMEM(class_offsets.shape, jnp.int32),
            columns,
            columns,
            vm((folds, GUARD + -(-positions // 8) * 8 + 8, LANES), f32),
            vm((folds, rows + 2 * STRIDE, LANES), f32),
            vm((folds, taller, LANES), f32),
            vm((3, rows, channels), f32),
            vm((images, rows, channels), f32),
            vm((images, 1, width), f32),
            vm((images, 8, LANES), f32),
            vm((images, 1, width), f32),
            vm((images, shards, 1, width), f32),
            vm((shards, width), f32),
            vm((shards, width + LANES), f32),
            vm((faces, 1), f32),
            vm((faces, classes), bf16),
            vm((faces, width), f32),
            vm((images, shards, 1, width), f32),
            vm((images, shards, 1, width), f32),
            vm((images, shards, 1, width + LANES), f32),
            vm((images, shards, 1, width + LANES), f32),
            dma((11,)),
            dma((images, 2)),
            dma((images, 2)),
            dma((images, 2)),
            dma((images, 2)),
            dma((3, images)),
            dma((3, images)),
        ],
        compiler_params=pltpu.CompilerParams(
            collective_id=0, has_side_effects=True, vmem_limit_bytes=60000 * 1024
        ),
        name="window",
    )(
        section_input.reshape(images, positions, folds, LANES).transpose(1, 2, 0, 3).reshape(lined),
        conv_one,
        conv_two,
        unit_gain,
        offset_bias,
        leak_slope,
        depthwise,
        embed_weight,
        class_centers,
        labels,
        class_offsets,
    )
    result = pl.pallas_call(
        emit,
        out_shape=jax.ShapeDtypeStruct(lined, bf16),
        in_specs=[vmem],
        out_specs=hbm,
        scratch_shapes=[dma],
        name="emit",
    )(pltpu.with_memory_space_constraint(result, pltpu.VMEM))
    result = result.reshape(positions, folds, images, LANES).transpose(2, 0, 1, 3)
    return result.reshape(1, micro, local, positions, channels)


def solution(mesh):
    placed = (
        P(None, "shard", None, None),
        P("section", None, None),
        P("section", None, None),
        P("section", None),
        P("section", None),
        P("section", None),
        P(),
        P(),
        P("shard", None),
        P(),
        P("shard"),
    )
    return jax.shard_map(
        on_device,
        mesh=mesh,
        in_specs=placed,
        out_specs=P("section", None, "shard", None, None),
        check_vma=False,
    )
```

```python
import functools
import math

import jax
import jax.numpy as jnp
from jax import lax
from jax.experimental import pallas as pl
from jax.experimental.pallas import tpu as pltpu
from jax.sharding import PartitionSpec as P

MESH = pl.DeviceIdType.MESH
STRIDE = 16
GUARD = 16
HALF_ROWS = 16
LANES = 128

margin_value = 0.4
scale_value = 64.0
tiny_value = 1e-06
lowest = -3e38

f32 = jnp.float32
bf16 = jnp.bfloat16


def dot(left, right):
    return jnp.dot(left, right, preferred_element_type=f32)


def kernel(
    sections,
    shards,
    images,
    side,
    x_hbm,
    w1_hbm,
    w2_hbm,
    gain_hbm,
    bias_hbm,
    leak_hbm,
    depth_hbm,
    embed_hbm,
    centre_hbm,
    labels_hbm,
    offset_hbm,
    out_ref,
    xraw,
    xall,
    xin,
    xsend,
    gin,
    gout,
    oall,
    w1,
    w2,
    w1t,
    w2t,
    gain_ref,
    bias_ref,
    leak_ref,
    depth,
    embed,
    embed_t,
    raw,
    centres,
    centres_t,
    labels_ref,
    offset_ref,
    cols_a,
    cols_b,
    spread,
    padded,
    packed,
    dws,
    slope,
    emb,
    scales,
    unit_src,
    unit_all,
    label_col,
    hits,
    picked,
    chosen_src,
    chosen_rcv,
    part_src,
    part_rcv,
    in_sem,
    xs_send,
    xs_recv,
    gs_send,
    gs_recv,
    peer_send,
    peer_recv,
):
    section = lax.axis_index("section")
    me = lax.axis_index("shard")
    first = section == 0
    last = section == sections - 1
    positions = side * side
    rows = side * STRIDE
    channels = w1.shape[1]
    folds = channels // LANES
    width = embed.shape[1]
    lines = width // LANES
    class_count = centres.shape[0]
    faces = images * shards
    body = pl.ds(STRIDE, rows)

    def bring(k, source, target):
        return pltpu.make_async_copy(source, target, in_sem.at[k])

    x_copy = bring(0, x_hbm, xraw)
    w1_copy = bring(1, w1_hbm.at[0], w1)
    w2_copy = bring(2, w2_hbm.at[0], w2)
    gain_copy = bring(3, gain_hbm, gain_ref)
    bias_copy = bring(4, bias_hbm, bias_ref)
    leak_copy = bring(5, leak_hbm, leak_ref)
    depth_copy = bring(6, depth_hbm, depth)
    embed_copy = bring(7, embed_hbm, embed)
    centre_copy = bring(8, centre_hbm, raw)
    labels_copy = bring(9, labels_hbm, labels_ref)
    offset_copy = bring(10, offset_hbm, offset_ref)

    @pl.when(first)
    def _():
        x_copy.start()

    @pl.when(last)
    def _():
        labels_copy.start()
        offset_copy.start()
        depth_copy.start()
        centre_copy.start()

    w1_copy.start()
    gain_copy.start()
    bias_copy.start()
    leak_copy.start()
    w2_copy.start()

    @pl.when(last)
    def _():
        embed_copy.start()

    barrier = pltpu.get_barrier_semaphore()

    @pl.when(section > 0)
    def _():
        pl.semaphore_signal(barrier, inc=1, device_id={"section": section - 1}, device_id_type=MESH)

    @pl.when(section < sections - 1)
    def _():
        pl.semaphore_signal(barrier, inc=1, device_id={"section": section + 1}, device_id_type=MESH)

    @pl.when(last)
    def _():
        for k in range(1, shards):
            peer = lax.rem(me + k, shards)
            pl.semaphore_signal(barrier, inc=1, device_id={"shard": peer}, device_id_type=MESH)

    neighbours = jnp.where(first, 0, 1) + jnp.where(last, shards - 1, 1)

    def greet():
        with jax.named_scope("barrier"):
            pl.semaphore_wait(barrier, neighbours)

    for cols in (cols_a, cols_b):
        cols[pl.ds(0, STRIDE), :] = jnp.zeros((STRIDE, 3 * channels), bf16)
        cols[pl.ds(rows + STRIDE, STRIDE), :] = jnp.zeros((STRIDE, 3 * channels), bf16)
    for h in range(folds):
        padded[h, pl.ds(0, STRIDE), :] = jnp.zeros((STRIDE, LANES), f32)
        padded[h, pl.ds(rows + STRIDE, STRIDE), :] = jnp.zeros((STRIDE, LANES), f32)
        spread[h, pl.ds(0, GUARD), :] = jnp.zeros((GUARD, LANES), f32)
        tail = spread.shape[1] - GUARD - positions
        spread[h, pl.ds(GUARD + positions, tail), :] = jnp.zeros((tail, LANES), f32)
        packed[h, pl.ds(packed.shape[1] - 8, 8), :] = jnp.zeros((8, LANES), f32)

    column = lax.broadcasted_iota(jnp.int32, (STRIDE, LANES), 0)
    inside = {
        -1: (column >= 1) & (column < side),
        0: column < side,
        1: column < side - 1,
    }
    keep = (lax.broadcasted_iota(jnp.int32, (rows, LANES), 0) & (STRIDE - 1)) < side

    def lanes(h):
        return slice(h * LANES, (h + 1) * LANES)

    def spread_in(source):
        for h in range(folds):
            spread[h, pl.ds(GUARD, positions), :] = source[pl.ds(0, positions), lanes(h)].astype(f32)

    def expand(store):
        for i in range(side):
            for d in (-1, 0, 1):
                for h in range(folds):
                    value = spread[h, pl.ds(GUARD + side * i + d, STRIDE), :]
                    store(i, d, h, jnp.where(inside[d], value, 0.0))

    def expand_cols():
        def store(i, d, h, value):
            target = pl.ds(channels * (d + 1) + LANES * h, LANES)
            cols_a[pl.ds(STRIDE * (i + 1), STRIDE), target] = value.astype(bf16)

        expand(store)

    def shift_cols(start, count):
        for h in range(folds):
            for d in (-1, 0, 1):
                target = pl.ds(channels * (d + 1) + LANES * h, LANES)
                source = padded[h, pl.ds(STRIDE + start + d, count), :]
                cols_b[pl.ds(STRIDE + start, count), target] = source.astype(bf16)

    def centre_of(start, count):
        return cols_a[pl.ds(STRIDE + start, count), pl.ds(channels, channels)].astype(f32)

    depth3 = 3 * channels

    def chain(cols, weights, start, count, taps):
        total = None
        for d in range(3):
            low, high = max(taps[0] - 3 * d, 0), min(taps[1] - 3 * d, 3)
            if low < high:
                left = cols[pl.ds(start + STRIDE * d, count), pl.ds(channels * low, channels * (high - low))]
                right = weights[pl.ds(depth3 * d + channels * low, channels * (high - low)), :]
                term = dot(left, right)
                total = term if total is None else total + term
        return total

    def conv(cols, weights, cut):
        for start, count, middle in ((0, cut, 5), (cut, rows - cut, 4)):
            one = chain(cols, weights, start, count, (0, middle))
            two = chain(cols, weights, start, count, (middle, 9))
            yield start, count, one + jnp.maximum(two, lowest)

    half_rows = side // 2 * STRIDE
    send_cut = side // 2 * side // 8 * 8
    parts = ((0, send_cut), (send_cut, packed.shape[1] - send_cut))

    def compact(start, value):
        for i in range(value.shape[0] // STRIDE):
            for h in range(folds):
                piece = value[STRIDE * i : STRIDE * (i + 1), lanes(h)]
                packed[h, pl.ds(side * (start // STRIDE + i), STRIDE), :] = piece

    def collect(m, start, value):
        for i in range(value.shape[0] // STRIDE):
            for h in range(folds):
                piece = value[STRIDE * i : STRIDE * (i + 1), lanes(h)]
                where = (side * (start // STRIDE + i) * folds + h) * images + m
                oall[pl.ds(where, STRIDE, stride=folds * images), :] = piece

    def packed_out(target, part):
        low, count = parts[part]
        for h in range(folds):
            target[pl.ds(low, count), pl.ds(LANES * h, LANES)] = packed[h, pl.ds(low, count), :].astype(bf16)

    def flip():
        with jax.named_scope("flip"):

            @pl.loop(0, 9)
            def _(t):
                there = pl.ds(pl.multiple_of(t * channels, channels), channels)
                here = pl.ds(pl.multiple_of((8 - t) * channels, channels), channels)
                w2t[there, :] = w2[here, :].T
                w1t[there, :] = w1[here, :].T

    sources = (unit_src, chosen_src, part_src)
    targets = (unit_all, chosen_rcv, part_rcv)

    def peer_copy(kind, m, to):
        source = sources[kind].at[m]
        return pltpu.make_async_remote_copy(
            src_ref=source if kind == 0 else source.at[to],
            dst_ref=targets[kind].at[m, me],
            send_sem=peer_send.at[kind, m],
            recv_sem=peer_recv.at[kind, m],
            device_id={"shard": to},
            device_id_type=MESH,
        )

    order = [k for k in range(3 * shards // 4, shards)] + [k for k in range(1, 3 * shards // 4)]

    def send_peers(kind, m):
        for k in order:
            peer_copy(kind, m, lax.rem(me + k, shards)).start()

    def peers_all(kind, m):
        others = targets[kind].at[m, pl.ds(0, shards - 1)]
        return pltpu.make_async_remote_copy(
            src_ref=others,
            dst_ref=others,
            send_sem=peer_send.at[kind, m],
            recv_sem=peer_recv.at[kind, m],
            device_id={"shard": lax.rem(me + 1, shards)},
            device_id_type=MESH,
        )

    def recv_peers(kind, m):
        peers_all(kind, m).wait_recv()

    def drain_peers(kind, m):
        peers_all(kind, m).wait_send()

    def x_send(m, part, step=1):
        window = pl.ds(*parts[part])
        return pltpu.make_async_remote_copy(
            src_ref=xsend.at[m, window],
            dst_ref=xin.at[m, window],
            send_sem=xs_send.at[m, part],
            recv_sem=xs_recv.at[m, part],
            device_id={"section": section + step},
            device_id_type=MESH,
        )

    def g_send(m, part, step=-1):
        window = pl.ds(*parts[part])
        return pltpu.make_async_remote_copy(
            src_ref=gout.at[m, window],
            dst_ref=gin.at[m, window],
            send_sem=gs_send.at[m, part],
            recv_sem=gs_recv.at[m, part],
            device_id={"section": section + step},
            device_id_type=MESH,
        )

    def receive(copy, m, step, landing):
        for part in range(2):
            copy(m, part, step).wait_recv()
        spread_in(landing.at[m])

    def forward(m, finish, between=None):
        gain = gain_ref[...]
        bias = bias_ref[...]
        leak = leak_ref[...]
        half = (0.5 * (1.0 - leak)) * gain
        base = leak * gain + half
        quarter = 0.25 * (1.0 - leak)
        for start, count, total in conv(cols_a, w1, half_rows + STRIDE):
            z = total * gain + bias
            turn = jnp.tanh(z + z)
            share = base + half * turn
            active = jnp.maximum(z, leak * z) - quarter * jnp.log(0.5 + 0.5 * jnp.abs(turn))
            mask = keep[:count]
            for h in range(folds):
                slope[m, pl.ds(start, count), lanes(h)] = jnp.where(mask, share[:, lanes(h)], 0.0)
                padded[h, pl.ds(STRIDE + start, count), :] = jnp.where(mask, active[:, lanes(h)], 0.0)
            shift_cols(start, count)
        if between is not None:
            between()
        for part, (start, count, total) in enumerate(list(conv(cols_b, w2, half_rows))):
            finish(part, start, centre_of(start, count) + total)

    def backward(m, finish):
        for start, count, total in conv(cols_a, w2t, half_rows + STRIDE):
            hidden = total * slope[m, pl.ds(start, count), :]
            for h in range(folds):
                padded[h, pl.ds(STRIDE + start, count), :] = hidden[:, lanes(h)]
            shift_cols(start, count)
        for part, (start, count, total) in enumerate(list(conv(cols_b, w1t, half_rows))):
            finish(part, start, centre_of(start, count) + total)

    def small_waits():
        gain_copy.wait()
        bias_copy.wait()
        leak_copy.wait()

    @pl.when(section < sections - 1)
    def _():
        @pl.when(first)
        def _():
            with jax.named_scope("w_wait"):
                x_copy.wait()
            xall[...] = xraw[...].astype(f32)

        small_waits()
        with jax.named_scope("w_wait"):
            w1_copy.wait()

        def run(m, peeled):
            @pl.when(first)
            def _():
                for h in range(folds):
                    spread[h, pl.ds(GUARD, positions), :] = xall[
                        pl.ds(h * images + m, positions, stride=folds * images), :
                    ]

            @pl.when(section > 0)
            def _():
                receive(x_send, m, -1, xin)

            expand_cols()

            def finish(part, start, value):
                compact(start, value)
                packed_out(xsend.at[m], part)
                if peeled and part == 0:
                    greet()
                x_send(m, part).start()

            forward(m, finish, w2_copy.wait if peeled else None)

        with jax.named_scope("forward"):
            run(0, True)

        @pl.loop(1, images)
        def _(m):
            with jax.named_scope("forward"):
                run(m, False)

        flip()

        @pl.loop(0, images)
        def _(m):
            with jax.named_scope("g_wait"):
                for part in range(2):
                    g_send(m, part, 1).wait_recv()
            with jax.named_scope("backward"):
                spread_in(gin.at[m])
                expand_cols()

                def finish(part, start, value):
                    compact(start, value)
                    collect(m, start, value)

                backward(m, finish)

                @pl.when(section > 0)
                def _():
                    for part in range(2):
                        packed_out(gout.at[m], part)
                        g_send(m, part).start()

    @pl.when(last)
    def _():
        labels_copy.wait()
        offset_copy.wait()
        micro = labels_ref.shape[0]
        local = images // micro
        row = lax.broadcasted_iota(jnp.int32, (shards, labels_ref.shape[1]), 0)
        lane = lax.broadcasted_iota(jnp.int32, (shards, labels_ref.shape[1]), 1)
        for m in range(micro):
            values = labels_ref[pl.ds(m, 1), :].astype(f32)
            for f in range(local):
                mine = jnp.where(lane == row * local + f, values, 0.0)
                label_col[pl.ds((m * local + f) * shards, shards), :] = jnp.sum(mine, axis=1, keepdims=True)
        ids = lax.broadcasted_iota(jnp.int32, (faces, class_count), 1)
        wanted = label_col[...].astype(jnp.int32) - offset_ref[0]
        hits[...] = jnp.where(wanted == ids, 1.0, 0.0).astype(bf16)

        depth_copy.wait()
        spread_in(depth)

        def store(i, d, h, value):
            dws[d + 1, pl.ds(STRIDE * i, STRIDE), pl.ds(LANES * h, LANES)] = value

        expand(store)
        with jax.named_scope("centre_wait"):
            centre_copy.wait()
        block = LANES

        @pl.loop(0, class_count // block)
        def _(b):
            part = pl.ds(pl.multiple_of(b * block, block), block)
            values = raw[part, :].astype(f32)
            square = jnp.mean(values * values, axis=-1, keepdims=True)
            factor = lax.rsqrt(square + tiny_value) / math.sqrt(width)
            normed = (values * factor).astype(bf16)
            centres[part, :] = normed
            centres_t[:, part] = normed.T

        picked[...] = dot(hits[...], centres[...])
        for m in range(images):
            for k in range(lines):
                chosen_src[m, :, k, :] = picked[pl.ds(m * shards, shards), lanes(k)]
            chosen_rcv[m, me] = chosen_src[m, me]
        embed_copy.wait()
        embed_t[...] = embed[...].T
        small_waits()
        with jax.named_scope("w_wait"):
            w1_copy.wait()
            w2_copy.wait()
        flip()
        greet()

        @pl.loop(0, images)
        def _(m):
            send_peers(1, m)

        def last_forward(m):
            with jax.named_scope("x_wait"):
                receive(x_send, m, -1, xin)
            expand_cols()
            sums = []

            def finish(part, start, value):
                weighted = value.astype(bf16).astype(f32) * dws[1, pl.ds(start, value.shape[0]), :]
                sums.append(jnp.sum(weighted, axis=0, keepdims=True))

            forward(m, finish)
            pooled = jnp.broadcast_to(sums[0] + sums[1], (HALF_ROWS, channels)).astype(bf16)
            embedded = dot(pooled, embed[...])[:1]
            square = jnp.mean(embedded * embedded, axis=-1, keepdims=True)
            factor = lax.rsqrt(square + tiny_value) / math.sqrt(width)
            normed = (embedded * factor).astype(bf16).astype(f32)
            for k in range(lines):
                unit_src[m, pl.ds(k, 1), :] = normed[:, lanes(k)]
            unit_all[m, me] = unit_src[m]
            send_peers(0, m)
            for k in range(lines):
                emb[m, pl.ds(k, 1), :] = embedded[:, lanes(k)]
            scales[m, pl.ds(0, 1), :] = jnp.broadcast_to(factor, (1, LANES))
            scales[m, pl.ds(1, 1), :] = jnp.broadcast_to(1.0 / (width * (square + tiny_value)), (1, LANES))

        def partial(m):
            with jax.named_scope("unit_wait"):
                recv_peers(0, m)
            flat = jnp.concatenate([unit_all[m, :, k, :] for k in range(lines)], axis=1)
            cosines = dot(flat.astype(bf16), centres_t[...])
            mine = pl.ds(pl.multiple_of(m * shards, shards), shards)
            logits = scale_value * (cosines - margin_value * hits[mine, :].astype(f32))
            grown = jnp.exp(logits)
            weighted = dot(grown.astype(bf16), centres[...])
            for k in range(lines):
                part_src[m, :, k, :] = weighted[:, lanes(k)]
            part_src[m, :, lines, :] = jnp.broadcast_to(
                jnp.sum(grown, axis=1, keepdims=True), (shards, LANES)
            )
            part_rcv[m, me] = part_src[m, me]
            send_peers(2, m)

        def last_backward(m):
            with jax.named_scope("chosen_wait"):
                recv_peers(1, m)
            chosen = jnp.sum(chosen_rcv[m], axis=0)
            with jax.named_scope("part_wait"):
                recv_peers(2, m)
            sums = jnp.sum(part_rcv[m], axis=0)
            grad_unit = scale_value * (sums[:lines] / sums[lines : lines + 1] - chosen)
            embedded = emb[m]
            factor = scales[m, 0:1, :]
            shrink = scales[m, 1:2, :]
            inner = jnp.sum(embedded * grad_unit, axis=0, keepdims=True)
            inner = jnp.sum(inner, axis=1, keepdims=True)
            grad_embed = factor * (grad_unit - embedded * (inner * shrink))
            grad_embed = jnp.concatenate(
                [jnp.broadcast_to(grad_embed[k : k + 1], (HALF_ROWS, LANES)) for k in range(lines)], axis=1
            ).astype(bf16)
            gpool = dot(grad_embed, embed_t[...])[:1]
            for d in range(3):
                cols_a[body, pl.ds(channels * d, channels)] = (gpool * dws[d]).astype(bf16)

            def finish(part, start, value):
                compact(start, value)
                packed_out(gout.at[m], part)
                g_send(m, part).start()
                collect(m, start, value)

            backward(m, finish)

        lag = 4

        @pl.loop(0, images + lag)
        def _(t):
            @pl.when(t < images)
            def _():
                with jax.named_scope("forward"):
                    last_forward(t)

            @pl.when((t >= 2) & (t < images + 2))
            def _():
                with jax.named_scope("partial"):
                    partial(t - 2)

            @pl.when(t >= lag)
            def _():
                with jax.named_scope("backward"):
                    last_backward(t - lag)

    with jax.named_scope("drain"):
        out_ref[...] = oall[pl.ds(0, positions * folds * images), :].astype(bf16)

        @pl.loop(0, images)
        def _(m):
            for part in range(2):

                @pl.when(section < sections - 1)
                def _():
                    x_send(m, part).wait_send()

                @pl.when(section > 0)
                def _():
                    g_send(m, part).wait_send()

        @pl.when(last)
        def _():
            @pl.loop(0, images)
            def _(m):
                for kind in range(3):
                    drain_peers(kind, m)


def emit(source, target, sem):
    copy = pltpu.make_async_copy(source, target, sem)
    copy.start()
    copy.wait()


def on_device(
    section_input,
    conv_one,
    conv_two,
    unit_gain,
    offset_bias,
    leak_slope,
    depthwise,
    embed_weight,
    class_centers,
    labels,
    class_offsets,
):
    sections = lax.axis_size("section")
    shards = lax.axis_size("shard")
    micro, local, positions, channels = section_input.shape
    side = math.isqrt(positions)
    images = micro * local
    rows = side * STRIDE
    folds = channels // LANES
    width = embed_weight.shape[1]
    lines = width // LANES
    classes = class_centers.shape[0]
    faces = shards * images
    hbm = pl.BlockSpec(memory_space=pltpu.HBM)
    vmem = pl.BlockSpec(memory_space=pltpu.VMEM)
    dma = pltpu.SemaphoreType.DMA
    vm = pltpu.VMEM
    lined = (positions * folds * images, LANES)
    taller = -(-(positions + STRIDE - side) // 8) * 8
    maps = vm((images, taller, channels), bf16)
    weights = vm(conv_one.shape[1:], bf16)
    columns = vm((rows + 2 * STRIDE, 3 * channels), bf16)
    row = vm((1, channels), f32)
    result = pl.pallas_call(
        functools.partial(kernel, sections, shards, images, side),
        out_shape=vm(lined, bf16),
        in_specs=[hbm] * 11,
        out_specs=vmem,
        scratch_shapes=[
            vm(lined, bf16),
            vm(lined, f32),
            maps,
            maps,
            maps,
            maps,
            vm(((positions + STRIDE - side) * folds * images, LANES), f32),
            weights,
            weights,
            weights,
            weights,
            row,
            row,
            row,
            vm((positions, channels), bf16),
            vm(embed_weight.shape, bf16),
            vm((width, channels), bf16),
            vm((classes, width), bf16),
            vm((classes, width), bf16),
            vm((width, classes), bf16),
            vm(labels.shape, jnp.int32),
            pltpu.SMEM(class_offsets.shape, jnp.int32),
            columns,
            columns,
            vm((folds, GUARD + -(-positions // 8) * 8 + 8, LANES), f32),
            vm((folds, rows + 2 * STRIDE, LANES), f32),
            vm((folds, taller, LANES), f32),
            vm((3, rows, channels), f32),
            vm((images, rows, channels), f32),
            vm((images, lines, LANES), f32),
            vm((images, 8, LANES), f32),
            vm((images, lines, LANES), f32),
            vm((images, shards, lines, LANES), f32),
            vm((faces, 1), f32),
            vm((faces, classes), bf16),
            vm((faces, width), f32),
            vm((images, shards, lines, LANES), f32),
            vm((images, shards, lines, LANES), f32),
            vm((images, shards, lines + 1, LANES), f32),
            vm((images, shards, lines + 1, LANES), f32),
            dma((11,)),
            dma((images, 2)),
            dma((images, 2)),
            dma((images, 2)),
            dma((images, 2)),
            dma((3, images)),
            dma((3, images)),
        ],
        compiler_params=pltpu.CompilerParams(
            collective_id=0, has_side_effects=True, vmem_limit_bytes=60000 * 1024
        ),
        name="window",
    )(
        section_input.reshape(images, positions, folds, LANES).transpose(1, 2, 0, 3).reshape(lined),
        conv_one,
        conv_two,
        unit_gain,
        offset_bias,
        leak_slope,
        depthwise,
        embed_weight,
        class_centers,
        labels,
        class_offsets,
    )
    result = pl.pallas_call(
        emit,
        out_shape=jax.ShapeDtypeStruct(lined, bf16),
        in_specs=[vmem],
        out_specs=hbm,
        scratch_shapes=[dma],
        name="emit",
    )(pltpu.with_memory_space_constraint(result, pltpu.VMEM))
    result = result.reshape(positions, folds, images, LANES).transpose(2, 0, 1, 3)
    return result.reshape(1, micro, local, positions, channels)


def solution(mesh):
    placed = (
        P(None, "shard", None, None),
        P("section", None, None),
        P("section", None, None),
        P("section", None),
        P("section", None),
        P("section", None),
        P(),
        P(),
        P("shard", None),
        P(),
        P("shard"),
    )
    return jax.shard_map(
        on_device,
        mesh=mesh,
        in_specs=placed,
        out_specs=P("section", None, "shard", None, None),
        check_vma=False,
    )
```

```python
import functools
import math

import jax
import jax.numpy as jnp
from jax import lax
from jax.experimental import pallas as pl
from jax.experimental.pallas import tpu as pltpu
from jax.sharding import PartitionSpec as P

MESH = pl.DeviceIdType.MESH
STRIDE = 16
GUARD = 16
HALF_ROWS = 16
LANES = 128

margin_value = 0.4
scale_value = 64.0
tiny_value = 1e-06
lowest = -3e38

f32 = jnp.float32
bf16 = jnp.bfloat16


def dot(left, right):
    return jnp.dot(left, right, preferred_element_type=f32)


def kernel(
    sections,
    shards,
    images,
    side,
    x_hbm,
    w1_hbm,
    w2_hbm,
    gain_hbm,
    bias_hbm,
    leak_hbm,
    depth_hbm,
    embed_hbm,
    centre_hbm,
    labels_hbm,
    offset_hbm,
    out_ref,
    xraw,
    xall,
    xin,
    xsend,
    gin,
    gout,
    oall,
    w1,
    w2,
    w1t,
    w2t,
    gain_ref,
    bias_ref,
    leak_ref,
    depth,
    embed,
    embed_t,
    raw,
    centres,
    centres_t,
    labels_ref,
    offset_ref,
    cols_a,
    cols_b,
    spread,
    padded,
    packed,
    dws,
    slope,
    emb,
    scales,
    unit_src,
    unit_all,
    flat,
    label_col,
    hits,
    picked,
    chosen_src,
    chosen_rcv,
    part_src,
    part_rcv,
    in_sem,
    xs_send,
    xs_recv,
    gs_send,
    gs_recv,
    peer_send,
    peer_recv,
):
    section = lax.axis_index("section")
    me = lax.axis_index("shard")
    first = section == 0
    last = section == sections - 1
    positions = side * side
    rows = side * STRIDE
    channels = w1.shape[1]
    folds = channels // LANES
    width = embed.shape[1]
    lines = width // LANES
    class_count = centres.shape[0]
    lead = max(shards // 8, 1)
    steps = images + 1
    ahead = me < lead
    faces = steps * shards
    body = pl.ds(STRIDE, rows)

    def bring(k, source, target):
        return pltpu.make_async_copy(source, target, in_sem.at[k])

    x_copy = bring(0, x_hbm, xraw)
    w1_copy = bring(1, w1_hbm.at[0], w1)
    w2_copy = bring(2, w2_hbm.at[0], w2)
    gain_copy = bring(3, gain_hbm, gain_ref)
    bias_copy = bring(4, bias_hbm, bias_ref)
    leak_copy = bring(5, leak_hbm, leak_ref)
    depth_copy = bring(6, depth_hbm, depth)
    embed_copy = bring(7, embed_hbm, embed)
    centre_copy = bring(8, centre_hbm, raw)
    labels_copy = bring(9, labels_hbm, labels_ref)
    offset_copy = bring(10, offset_hbm, offset_ref)

    @pl.when(first)
    def _():
        x_copy.start()

    @pl.when(last)
    def _():
        labels_copy.start()
        offset_copy.start()
        depth_copy.start()
        centre_copy.start()

    w1_copy.start()
    gain_copy.start()
    bias_copy.start()
    leak_copy.start()
    w2_copy.start()

    @pl.when(last)
    def _():
        embed_copy.start()

    barrier = pltpu.get_barrier_semaphore()

    @pl.when(section > 0)
    def _():
        pl.semaphore_signal(barrier, inc=1, device_id={"section": section - 1}, device_id_type=MESH)

    @pl.when(section < sections - 1)
    def _():
        pl.semaphore_signal(barrier, inc=1, device_id={"section": section + 1}, device_id_type=MESH)

    @pl.when(last)
    def _():
        for k in range(1, shards):
            peer = lax.rem(me + k, shards)
            pl.semaphore_signal(barrier, inc=1, device_id={"shard": peer}, device_id_type=MESH)

    neighbours = jnp.where(first, 0, 1) + jnp.where(last, shards - 1, 1)

    def greet():
        with jax.named_scope("barrier"):
            pl.semaphore_wait(barrier, neighbours)

    for cols in (cols_a, cols_b):
        cols[pl.ds(0, STRIDE), :] = jnp.zeros((STRIDE, 3 * channels), bf16)
        cols[pl.ds(rows + STRIDE, STRIDE), :] = jnp.zeros((STRIDE, 3 * channels), bf16)
    for h in range(folds):
        padded[h, pl.ds(0, STRIDE), :] = jnp.zeros((STRIDE, LANES), f32)
        padded[h, pl.ds(rows + STRIDE, STRIDE), :] = jnp.zeros((STRIDE, LANES), f32)
        spread[h, pl.ds(0, GUARD), :] = jnp.zeros((GUARD, LANES), f32)
        tail = spread.shape[1] - GUARD - positions
        spread[h, pl.ds(GUARD + positions, tail), :] = jnp.zeros((tail, LANES), f32)
        packed[h, pl.ds(packed.shape[1] - 8, 8), :] = jnp.zeros((8, LANES), f32)

    column = lax.broadcasted_iota(jnp.int32, (STRIDE, LANES), 0)
    inside = {
        -1: (column >= 1) & (column < side),
        0: column < side,
        1: column < side - 1,
    }
    keep = (lax.broadcasted_iota(jnp.int32, (rows, LANES), 0) & (STRIDE - 1)) < side

    def lanes(h):
        return slice(h * LANES, (h + 1) * LANES)

    def spread_in(source):
        for h in range(folds):
            spread[h, pl.ds(GUARD, positions), :] = source[pl.ds(0, positions), lanes(h)].astype(f32)

    def expand(store):
        for i in range(side):
            for d in (-1, 0, 1):
                for h in range(folds):
                    value = spread[h, pl.ds(GUARD + side * i + d, STRIDE), :]
                    store(i, d, h, jnp.where(inside[d], value, 0.0))

    def expand_cols():
        def store(i, d, h, value):
            target = pl.ds(channels * (d + 1) + LANES * h, LANES)
            cols_a[pl.ds(STRIDE * (i + 1), STRIDE), target] = value.astype(bf16)

        expand(store)

    def shift_cols(start, count):
        for h in range(folds):
            for d in (-1, 0, 1):
                target = pl.ds(channels * (d + 1) + LANES * h, LANES)
                source = padded[h, pl.ds(STRIDE + start + d, count), :]
                cols_b[pl.ds(STRIDE + start, count), target] = source.astype(bf16)

    def centre_of(start, count):
        return cols_a[pl.ds(STRIDE + start, count), pl.ds(channels, channels)].astype(f32)

    depth3 = 3 * channels

    def chain(cols, weights, start, count, taps):
        total = None
        for d in range(3):
            low, high = max(taps[0] - 3 * d, 0), min(taps[1] - 3 * d, 3)
            if low < high:
                left = cols[pl.ds(start + STRIDE * d, count), pl.ds(channels * low, channels * (high - low))]
                right = weights[pl.ds(depth3 * d + channels * low, channels * (high - low)), :]
                term = dot(left, right)
                total = term if total is None else total + term
        return total

    def conv(cols, weights, cut):
        for start, count, middle in ((0, cut, 5), (cut, rows - cut, 4)):
            one = chain(cols, weights, start, count, (0, middle))
            two = chain(cols, weights, start, count, (middle, 9))
            yield start, count, one + jnp.maximum(two, lowest)

    half_rows = side // 2 * STRIDE
    send_cut = side // 2 * side // 8 * 8
    parts = ((0, send_cut), (send_cut, packed.shape[1] - send_cut))

    def compact(start, value):
        for i in range(value.shape[0] // STRIDE):
            for h in range(folds):
                piece = value[STRIDE * i : STRIDE * (i + 1), lanes(h)]
                packed[h, pl.ds(side * (start // STRIDE + i), STRIDE), :] = piece

    def collect(m, start, value):
        for i in range(value.shape[0] // STRIDE):
            for h in range(folds):
                piece = value[STRIDE * i : STRIDE * (i + 1), lanes(h)]
                where = (side * (start // STRIDE + i) * folds + h) * images + m
                oall[pl.ds(where, STRIDE, stride=folds * images), :] = piece

    def packed_out(target, part):
        low, count = parts[part]
        for h in range(folds):
            target[pl.ds(low, count), pl.ds(LANES * h, LANES)] = packed[h, pl.ds(low, count), :].astype(bf16)

    def flip():
        with jax.named_scope("flip"):

            @pl.loop(0, 9)
            def _(t):
                there = pl.ds(pl.multiple_of(t * channels, channels), channels)
                here = pl.ds(pl.multiple_of((8 - t) * channels, channels), channels)
                w2t[there, :] = w2[here, :].T
                w1t[there, :] = w1[here, :].T

    order = [k for k in range(3 * shards // 4, shards)] + [k for k in range(1, 3 * shards // 4)]

    def peer_copy(kind, m, to, source, target):
        return pltpu.make_async_remote_copy(
            src_ref=source,
            dst_ref=target.at[m, me],
            send_sem=peer_send.at[kind, m],
            recv_sem=peer_recv.at[jnp.where(ahead, 0, 3) if kind == 0 else kind, m],
            device_id={"shard": to},
            device_id_type=MESH,
        )

    def send_units(m):
        for k in order:
            peer_copy(0, m, lax.rem(me + k, shards), unit_src.at[m], unit_all).start()

    def send_chosen(m):
        for k in order:
            to = lax.rem(me + k, shards)
            peer_copy(1, m, to, chosen_src.at[m, to], chosen_rcv).start()

    def send_sums(p, m, low, high):
        for n in range(low, high):

            @pl.when(me != n)
            def _():
                peer_copy(2, m, n, part_src.at[p, n], part_rcv).start()

            @pl.when(me == n)
            def _():
                part_rcv[m, n] = part_src[p, n]

    def arrivals(kind, m, target, count, sem):
        others = target.at[m, pl.ds(0, count)]
        return pltpu.make_async_remote_copy(
            src_ref=others,
            dst_ref=others,
            send_sem=peer_send.at[kind, m],
            recv_sem=peer_recv.at[sem, m],
            device_id={"shard": lax.rem(me + 1, shards)},
            device_id_type=MESH,
        )

    def units_from(m, sem, members, mine):
        @pl.when(mine)
        def _():
            if members > 1:
                arrivals(0, m, unit_all, members - 1, sem).wait_recv()

        @pl.when(jnp.logical_not(mine))
        def _():
            arrivals(0, m, unit_all, members, sem).wait_recv()

    def x_send(m, part, step=1):
        window = pl.ds(*parts[part])
        return pltpu.make_async_remote_copy(
            src_ref=xsend.at[m, window],
            dst_ref=xin.at[m, window],
            send_sem=xs_send.at[m, part],
            recv_sem=xs_recv.at[m, part],
            device_id={"section": section + step},
            device_id_type=MESH,
        )

    def g_send(m, part, step=-1):
        window = pl.ds(*parts[part])
        return pltpu.make_async_remote_copy(
            src_ref=gout.at[m, window],
            dst_ref=gin.at[m, window],
            send_sem=gs_send.at[m, part],
            recv_sem=gs_recv.at[m, part],
            device_id={"section": section + step},
            device_id_type=MESH,
        )

    def receive(copy, m, step, landing):
        for part in range(2):
            copy(m, part, step).wait_recv()
        spread_in(landing.at[m])

    def forward(m, finish, between=None):
        gain = gain_ref[...]
        bias = bias_ref[...]
        leak = leak_ref[...]
        half = (0.5 * (1.0 - leak)) * gain
        base = leak * gain + half
        quarter = 0.25 * (1.0 - leak)
        for start, count, total in conv(cols_a, w1, half_rows + STRIDE):
            z = total * gain + bias
            turn = jnp.tanh(z + z)
            share = base + half * turn
            active = jnp.maximum(z, leak * z) - quarter * jnp.log(0.5 + 0.5 * jnp.abs(turn))
            mask = keep[:count]
            for h in range(folds):
                slope[m, pl.ds(start, count), lanes(h)] = jnp.where(mask, share[:, lanes(h)], 0.0)
                padded[h, pl.ds(STRIDE + start, count), :] = jnp.where(mask, active[:, lanes(h)], 0.0)
            shift_cols(start, count)
        if between is not None:
            between()
        for part, (start, count, total) in enumerate(list(conv(cols_b, w2, half_rows))):
            finish(part, start, centre_of(start, count) + total)

    def backward(m, finish):
        for start, count, total in conv(cols_a, w2t, half_rows + STRIDE):
            hidden = total * slope[m, pl.ds(start, count), :]
            for h in range(folds):
                padded[h, pl.ds(STRIDE + start, count), :] = hidden[:, lanes(h)]
            shift_cols(start, count)
        for part, (start, count, total) in enumerate(list(conv(cols_b, w1t, half_rows))):
            finish(part, start, centre_of(start, count) + total)

    def small_waits():
        gain_copy.wait()
        bias_copy.wait()
        leak_copy.wait()

    @pl.when(section < sections - 1)
    def _():
        @pl.when(first)
        def _():
            with jax.named_scope("w_wait"):
                x_copy.wait()
            xall[...] = xraw[...].astype(f32)

        small_waits()
        with jax.named_scope("w_wait"):
            w1_copy.wait()

        def run(m, peeled):
            @pl.when(first)
            def _():
                for h in range(folds):
                    spread[h, pl.ds(GUARD, positions), :] = xall[
                        pl.ds(h * images + m, positions, stride=folds * images), :
                    ]

            @pl.when(section > 0)
            def _():
                receive(x_send, m, -1, xin)

            expand_cols()

            def finish(part, start, value):
                compact(start, value)
                packed_out(xsend.at[m], part)
                if peeled and part == 0:
                    greet()
                x_send(m, part).start()

            forward(m, finish, w2_copy.wait if peeled else None)

        with jax.named_scope("forward"):
            run(0, True)

        @pl.loop(1, images)
        def _(m):
            with jax.named_scope("forward"):
                run(m, False)

        flip()

        @pl.loop(0, images)
        def _(m):
            with jax.named_scope("g_wait"):
                for part in range(2):
                    g_send(m, part, 1).wait_recv()
            with jax.named_scope("backward"):
                spread_in(gin.at[m])
                expand_cols()

                def finish(part, start, value):
                    compact(start, value)
                    collect(m, start, value)

                backward(m, finish)

                @pl.when(section > 0)
                def _():
                    for part in range(2):
                        packed_out(gout.at[m], part)
                        g_send(m, part).start()

    @pl.when(last)
    def _():
        labels_copy.wait()
        offset_copy.wait()
        micro = labels_ref.shape[0]
        local = images // micro
        row = lax.broadcasted_iota(jnp.int32, (shards, labels_ref.shape[1]), 0)
        lane = lax.broadcasted_iota(jnp.int32, (shards, labels_ref.shape[1]), 1)
        wanted_by = []
        for m in range(micro):
            values = labels_ref[pl.ds(m, 1), :].astype(f32)
            for f in range(local):
                mine = jnp.where(lane == row * local + f, values, 0.0)
                wanted_by.append(jnp.sum(mine, axis=1, keepdims=True))
        front = lax.broadcasted_iota(jnp.int32, (shards, 1), 0) < lead
        for p in range(steps):
            early = wanted_by[min(p, images - 1)]
            label_col[pl.ds(p * shards, shards), :] = jnp.where(front, early, wanted_by[max(p - 1, 0)])
        ids = lax.broadcasted_iota(jnp.int32, (faces, class_count), 1)
        wanted = label_col[...].astype(jnp.int32) - offset_ref[0]
        hits[...] = jnp.where(wanted == ids, 1.0, 0.0).astype(bf16)

        depth_copy.wait()
        spread_in(depth)

        def store(i, d, h, value):
            dws[d + 1, pl.ds(STRIDE * i, STRIDE), pl.ds(LANES * h, LANES)] = value

        expand(store)
        with jax.named_scope("centre_wait"):
            centre_copy.wait()
        block = LANES

        @pl.loop(0, class_count // block)
        def _(b):
            part = pl.ds(pl.multiple_of(b * block, block), block)
            values = raw[part, :].astype(f32)
            square = jnp.mean(values * values, axis=-1, keepdims=True)
            factor = lax.rsqrt(square + tiny_value) / math.sqrt(width)
            normed = (values * factor).astype(bf16)
            centres[part, :] = normed
            centres_t[:, part] = normed.T

        picked[...] = dot(hits[...], centres[...])
        for m in range(images):
            for k in range(lines):
                chosen_src[m, pl.ds(0, lead), k, :] = picked[pl.ds(m * shards, lead), lanes(k)]
                chosen_src[m, pl.ds(lead, shards - lead), k, :] = picked[
                    pl.ds((m + 1) * shards + lead, shards - lead), lanes(k)
                ]
            chosen_rcv[m, me] = chosen_src[m, me]
        flat[...] = jnp.zeros_like(flat)
        embed_copy.wait()
        embed_t[...] = embed[...].T
        small_waits()
        with jax.named_scope("w_wait"):
            w1_copy.wait()
            w2_copy.wait()
        flip()
        greet()

        @pl.loop(0, images)
        def _(m):
            send_chosen(m)

        def last_forward(m):
            with jax.named_scope("x_wait"):
                receive(x_send, m, -1, xin)
            expand_cols()
            sums = []

            def finish(part, start, value):
                weighted = value.astype(bf16).astype(f32) * dws[1, pl.ds(start, value.shape[0]), :]
                sums.append(jnp.sum(weighted, axis=0, keepdims=True))

            forward(m, finish)
            pooled = jnp.broadcast_to(sums[0] + sums[1], (HALF_ROWS, channels)).astype(bf16)
            embedded = dot(pooled, embed[...])[:1]
            square = jnp.mean(embedded * embedded, axis=-1, keepdims=True)
            factor = lax.rsqrt(square + tiny_value) / math.sqrt(width)
            normed = (embedded * factor).astype(bf16).astype(f32)
            for k in range(lines):
                unit_src[m, pl.ds(k, 1), :] = normed[:, lanes(k)]
            unit_all[m, me] = unit_src[m]
            send_units(m)
            for k in range(lines):
                emb[m, pl.ds(k, 1), :] = embedded[:, lanes(k)]
            scales[m, pl.ds(0, 1), :] = jnp.broadcast_to(factor, (1, LANES))
            scales[m, pl.ds(1, 1), :] = jnp.broadcast_to(1.0 / (width * (square + tiny_value)), (1, LANES))

        def partial(p):
            with jax.named_scope("unit_wait"):

                @pl.when(p < images)
                def _():
                    units_from(p, 0, lead, ahead)
                    for k in range(lines):
                        flat[pl.ds(0, lead), lanes(k)] = unit_all[p, pl.ds(0, lead), k, :]

                @pl.when(p > 0)
                def _():
                    units_from(p - 1, 3, shards - lead, jnp.logical_not(ahead))
                    for k in range(lines):
                        flat[pl.ds(lead, shards - lead), lanes(k)] = unit_all[
                            p - 1, pl.ds(lead, shards - lead), k, :
                        ]

            cosines = dot(flat[...].astype(bf16), centres_t[...])
            mine = pl.ds(pl.multiple_of(p * shards, shards), shards)
            logits = scale_value * (cosines - margin_value * hits[mine, :].astype(f32))
            grown = jnp.exp(logits)
            weighted = dot(grown.astype(bf16), centres[...])
            for k in range(lines):
                part_src[p, :, k, :] = weighted[:, lanes(k)]
            part_src[p, :, lines, :] = jnp.broadcast_to(
                jnp.sum(grown, axis=1, keepdims=True), (shards, LANES)
            )

            @pl.when(p < images)
            def _():
                send_sums(p, p, 0, lead)

            @pl.when(p > 0)
            def _():
                send_sums(p, p - 1, lead, shards)

        def last_backward(m):
            with jax.named_scope("chosen_wait"):
                arrivals(1, m, chosen_rcv, shards - 1, 1).wait_recv()
            chosen = jnp.sum(chosen_rcv[m], axis=0)
            with jax.named_scope("part_wait"):
                arrivals(2, m, part_rcv, shards - 1, 2).wait_recv()
            sums = jnp.sum(part_rcv[m], axis=0)
            grad_unit = scale_value * (sums[:lines] / sums[lines : lines + 1] - chosen)
            embedded = emb[m]
            factor = scales[m, 0:1, :]
            shrink = scales[m, 1:2, :]
            inner = jnp.sum(embedded * grad_unit, axis=0, keepdims=True)
            inner = jnp.sum(inner, axis=1, keepdims=True)
            grad_embed = factor * (grad_unit - embedded * (inner * shrink))
            grad_embed = jnp.concatenate(
                [jnp.broadcast_to(grad_embed[k : k + 1], (HALF_ROWS, LANES)) for k in range(lines)], axis=1
            ).astype(bf16)
            gpool = dot(grad_embed, embed_t[...])[:1]
            for d in range(3):
                cols_a[body, pl.ds(channels * d, channels)] = (gpool * dws[d]).astype(bf16)

            def finish(part, start, value):
                compact(start, value)
                packed_out(gout.at[m], part)
                g_send(m, part).start()
                collect(m, start, value)

            backward(m, finish)

        lag = 4

        @pl.loop(0, images + lag)
        def _(t):
            @pl.when(t < images)
            def _():
                with jax.named_scope("forward"):
                    last_forward(t)

            @pl.when(
                (ahead & ((t == 1) | ((t >= 3) & (t < images + 3))))
                | (jnp.logical_not(ahead) & (t >= 1) & (t < images + 2))
            )
            def _():
                with jax.named_scope("partial"):
                    partial(jnp.where(ahead & (t > 1), t - 2, t - 1))

            @pl.when(t >= lag)
            def _():
                with jax.named_scope("backward"):
                    last_backward(t - lag)

    with jax.named_scope("drain"):
        out_ref[...] = oall[pl.ds(0, positions * folds * images), :].astype(bf16)

        @pl.loop(0, images)
        def _(m):
            for part in range(2):

                @pl.when(section < sections - 1)
                def _():
                    x_send(m, part).wait_send()

                @pl.when(section > 0)
                def _():
                    g_send(m, part).wait_send()

        @pl.when(last)
        def _():
            @pl.loop(0, images)
            def _(m):
                arrivals(0, m, unit_all, shards - 1, 0).wait_send()
                arrivals(1, m, chosen_rcv, shards - 1, 1).wait_send()
                arrivals(2, m, part_rcv, shards - 1, 2).wait_send()


def emit(source, target, sem):
    copy = pltpu.make_async_copy(source, target, sem)
    copy.start()
    copy.wait()


def on_device(
    section_input,
    conv_one,
    conv_two,
    unit_gain,
    offset_bias,
    leak_slope,
    depthwise,
    embed_weight,
    class_centers,
    labels,
    class_offsets,
):
    sections = lax.axis_size("section")
    shards = lax.axis_size("shard")
    micro, local, positions, channels = section_input.shape
    side = math.isqrt(positions)
    images = micro * local
    rows = side * STRIDE
    folds = channels // LANES
    width = embed_weight.shape[1]
    lines = width // LANES
    classes = class_centers.shape[0]
    faces = shards * (images + 1)
    hbm = pl.BlockSpec(memory_space=pltpu.HBM)
    vmem = pl.BlockSpec(memory_space=pltpu.VMEM)
    dma = pltpu.SemaphoreType.DMA
    vm = pltpu.VMEM
    lined = (positions * folds * images, LANES)
    taller = -(-(positions + STRIDE - side) // 8) * 8
    maps = vm((images, taller, channels), bf16)
    weights = vm(conv_one.shape[1:], bf16)
    columns = vm((rows + 2 * STRIDE, 3 * channels), bf16)
    row = vm((1, channels), f32)
    result = pl.pallas_call(
        functools.partial(kernel, sections, shards, images, side),
        out_shape=vm(lined, bf16),
        in_specs=[hbm] * 11,
        out_specs=vmem,
        scratch_shapes=[
            vm(lined, bf16),
            vm(lined, f32),
            maps,
            maps,
            maps,
            maps,
            vm(((positions + STRIDE - side) * folds * images, LANES), f32),
            weights,
            weights,
            weights,
            weights,
            row,
            row,
            row,
            vm((positions, channels), bf16),
            vm(embed_weight.shape, bf16),
            vm((width, channels), bf16),
            vm((classes, width), bf16),
            vm((classes, width), bf16),
            vm((width, classes), bf16),
            vm(labels.shape, jnp.int32),
            pltpu.SMEM(class_offsets.shape, jnp.int32),
            columns,
            columns,
            vm((folds, GUARD + -(-positions // 8) * 8 + 8, LANES), f32),
            vm((folds, rows + 2 * STRIDE, LANES), f32),
            vm((folds, taller, LANES), f32),
            vm((3, rows, channels), f32),
            vm((images, rows, channels), f32),
            vm((images, lines, LANES), f32),
            vm((images, 8, LANES), f32),
            vm((images, lines, LANES), f32),
            vm((images, shards, lines, LANES), f32),
            vm((shards, width), f32),
            vm((faces, 1), f32),
            vm((faces, classes), bf16),
            vm((faces, width), f32),
            vm((images, shards, lines, LANES), f32),
            vm((images, shards, lines, LANES), f32),
            vm((images + 1, shards, lines + 1, LANES), f32),
            vm((images, shards, lines + 1, LANES), f32),
            dma((11,)),
            dma((images, 2)),
            dma((images, 2)),
            dma((images, 2)),
            dma((images, 2)),
            dma((3, images)),
            dma((4, images)),
        ],
        compiler_params=pltpu.CompilerParams(
            collective_id=0, has_side_effects=True, vmem_limit_bytes=60000 * 1024
        ),
        name="window",
    )(
        section_input.reshape(images, positions, folds, LANES).transpose(1, 2, 0, 3).reshape(lined),
        conv_one,
        conv_two,
        unit_gain,
        offset_bias,
        leak_slope,
        depthwise,
        embed_weight,
        class_centers,
        labels,
        class_offsets,
    )
    result = pl.pallas_call(
        emit,
        out_shape=jax.ShapeDtypeStruct(lined, bf16),
        in_specs=[vmem],
        out_specs=hbm,
        scratch_shapes=[dma],
        name="emit",
    )(pltpu.with_memory_space_constraint(result, pltpu.VMEM))
    result = result.reshape(positions, folds, images, LANES).transpose(2, 0, 1, 3)
    return result.reshape(1, micro, local, positions, channels)


def solution(mesh):
    placed = (
        P(None, "shard", None, None),
        P("section", None, None),
        P("section", None, None),
        P("section", None),
        P("section", None),
        P("section", None),
        P(),
        P(),
        P("shard", None),
        P(),
        P("shard"),
    )
    return jax.shard_map(
        on_device,
        mesh=mesh,
        in_specs=placed,
        out_specs=P("section", None, "shard", None, None),
        check_vma=False,
    )
```

```python
import functools
import math

import jax
import jax.numpy as jnp
from jax import lax
from jax.experimental import pallas as pl
from jax.experimental.pallas import tpu as pltpu
from jax.sharding import PartitionSpec as P

MESH = pl.DeviceIdType.MESH
STRIDE = 16
GUARD = 16
HALF_ROWS = 16
LANES = 128

margin_value = 0.4
scale_value = 64.0
tiny_value = 1e-06
lowest = -3e38

f32 = jnp.float32
bf16 = jnp.bfloat16


def dot(left, right):
    return jnp.dot(left, right, preferred_element_type=f32)


def kernel(
    sections,
    shards,
    images,
    side,
    x_hbm,
    w1_hbm,
    w2_hbm,
    gain_hbm,
    bias_hbm,
    leak_hbm,
    depth_hbm,
    embed_hbm,
    centre_hbm,
    labels_hbm,
    offset_hbm,
    out_ref,
    xraw,
    xall,
    xin,
    xsend,
    gin,
    gout,
    oall,
    w1,
    w2,
    w1t,
    w2t,
    gain_ref,
    bias_ref,
    leak_ref,
    depth,
    embed,
    embed_t,
    raw,
    centres,
    centres_t,
    labels_ref,
    offset_ref,
    cols_a,
    cols_b,
    spread,
    padded,
    packed,
    dws,
    slope,
    emb,
    scales,
    unit_src,
    unit_all,
    flat,
    label_col,
    hits,
    picked,
    chosen_src,
    chosen_rcv,
    part_src,
    part_rcv,
    in_sem,
    xs_send,
    xs_recv,
    gs_send,
    gs_recv,
    peer_send,
    peer_recv,
):
    section = lax.axis_index("section")
    me = lax.axis_index("shard")
    first = section == 0
    last = section == sections - 1
    positions = side * side
    rows = side * STRIDE
    channels = w1.shape[1]
    folds = channels // LANES
    width = embed.shape[1]
    lines = width // LANES
    class_count = centres.shape[0]
    lead = max(shards // 8, 1)
    steps = images + 1
    ahead = me < lead
    faces = steps * shards
    body = pl.ds(STRIDE, rows)

    def bring(k, source, target):
        return pltpu.make_async_copy(source, target, in_sem.at[k])

    x_copy = bring(0, x_hbm, xraw)
    w1_copy = bring(1, w1_hbm.at[0], w1)
    w2_copy = bring(2, w2_hbm.at[0], w2)
    gain_copy = bring(3, gain_hbm, gain_ref)
    bias_copy = bring(4, bias_hbm, bias_ref)
    leak_copy = bring(5, leak_hbm, leak_ref)
    depth_copy = bring(6, depth_hbm, depth)
    embed_copy = bring(7, embed_hbm, embed)
    centre_copy = bring(8, centre_hbm, raw)
    labels_copy = bring(9, labels_hbm, labels_ref)
    offset_copy = bring(10, offset_hbm, offset_ref)

    @pl.when(first)
    def _():
        x_copy.start()

    @pl.when(last)
    def _():
        labels_copy.start()
        offset_copy.start()
        depth_copy.start()
        centre_copy.start()

    w1_copy.start()
    gain_copy.start()
    bias_copy.start()
    leak_copy.start()
    w2_copy.start()

    @pl.when(last)
    def _():
        embed_copy.start()

    barrier = pltpu.get_barrier_semaphore()

    @pl.when(section > 0)
    def _():
        pl.semaphore_signal(barrier, inc=1, device_id={"section": section - 1}, device_id_type=MESH)

    @pl.when(section < sections - 1)
    def _():
        pl.semaphore_signal(barrier, inc=1, device_id={"section": section + 1}, device_id_type=MESH)

    @pl.when(last)
    def _():
        for k in range(1, shards):
            peer = lax.rem(me + k, shards)
            pl.semaphore_signal(barrier, inc=1, device_id={"shard": peer}, device_id_type=MESH)

    neighbours = jnp.where(first, 0, 1) + jnp.where(last, shards - 1, 1)

    def greet():
        with jax.named_scope("barrier"):
            pl.semaphore_wait(barrier, neighbours)

    for cols in (cols_a, cols_b):
        cols[pl.ds(0, STRIDE), :] = jnp.zeros((STRIDE, 3 * channels), bf16)
        cols[pl.ds(rows + STRIDE, STRIDE), :] = jnp.zeros((STRIDE, 3 * channels), bf16)
    for h in range(folds):
        padded[h, pl.ds(0, STRIDE), :] = jnp.zeros((STRIDE, LANES), f32)
        padded[h, pl.ds(rows + STRIDE, STRIDE), :] = jnp.zeros((STRIDE, LANES), f32)
        spread[h, pl.ds(0, GUARD), :] = jnp.zeros((GUARD, LANES), f32)
        tail = spread.shape[1] - GUARD - positions
        spread[h, pl.ds(GUARD + positions, tail), :] = jnp.zeros((tail, LANES), f32)
        packed[h, pl.ds(packed.shape[1] - 8, 8), :] = jnp.zeros((8, LANES), f32)

    column = lax.broadcasted_iota(jnp.int32, (STRIDE, LANES), 0)
    inside = {
        -1: (column >= 1) & (column < side),
        0: column < side,
        1: column < side - 1,
    }
    keep = (lax.broadcasted_iota(jnp.int32, (rows, LANES), 0) & (STRIDE - 1)) < side

    def lanes(h):
        return slice(h * LANES, (h + 1) * LANES)

    def spread_in(source):
        for h in range(folds):
            spread[h, pl.ds(GUARD, positions), :] = source[pl.ds(0, positions), lanes(h)].astype(f32)

    def expand(store):
        for i in range(side):
            for d in (-1, 0, 1):
                for h in range(folds):
                    value = spread[h, pl.ds(GUARD + side * i + d, STRIDE), :]
                    store(i, d, h, jnp.where(inside[d], value, 0.0))

    def expand_cols():
        def store(i, d, h, value):
            target = pl.ds(channels * (d + 1) + LANES * h, LANES)
            cols_a[pl.ds(STRIDE * (i + 1), STRIDE), target] = value.astype(bf16)

        expand(store)

    def shift_cols(start, count):
        for h in range(folds):
            for d in (-1, 0, 1):
                target = pl.ds(channels * (d + 1) + LANES * h, LANES)
                source = padded[h, pl.ds(STRIDE + start + d, count), :]
                cols_b[pl.ds(STRIDE + start, count), target] = source.astype(bf16)

    def centre_of(start, count):
        return cols_a[pl.ds(STRIDE + start, count), pl.ds(channels, channels)].astype(f32)

    depth3 = 3 * channels

    def chain(cols, weights, start, count, taps):
        total = None
        for d in range(3):
            low, high = max(taps[0] - 3 * d, 0), min(taps[1] - 3 * d, 3)
            if low < high:
                left = cols[pl.ds(start + STRIDE * d, count), pl.ds(channels * low, channels * (high - low))]
                right = weights[pl.ds(depth3 * d + channels * low, channels * (high - low)), :]
                term = dot(left, right)
                total = term if total is None else total + term
        return total

    def conv(cols, weights, cut):
        for start, count, middle in ((0, cut, 5), (cut, rows - cut, 4)):
            one = chain(cols, weights, start, count, (0, middle))
            two = chain(cols, weights, start, count, (middle, 9))
            yield start, count, one + jnp.maximum(two, lowest)

    half_rows = side // 2 * STRIDE
    send_cut = side // 2 * side // 8 * 8
    parts = ((0, send_cut), (send_cut, packed.shape[1] - send_cut))

    def compact(start, value):
        for i in range(value.shape[0] // STRIDE):
            for h in range(folds):
                piece = value[STRIDE * i : STRIDE * (i + 1), lanes(h)]
                packed[h, pl.ds(side * (start // STRIDE + i), STRIDE), :] = piece

    def collect(m, start, value):
        for i in range(value.shape[0] // STRIDE):
            for h in range(folds):
                piece = value[STRIDE * i : STRIDE * (i + 1), lanes(h)]
                where = (side * (start // STRIDE + i) * folds + h) * images + m
                oall[pl.ds(where, STRIDE, stride=folds * images), :] = piece

    def packed_out(target, part):
        low, count = parts[part]
        for h in range(folds):
            target[pl.ds(low, count), pl.ds(LANES * h, LANES)] = packed[h, pl.ds(low, count), :].astype(bf16)

    def flip():
        with jax.named_scope("flip"):

            @pl.loop(0, 9)
            def _(t):
                there = pl.ds(pl.multiple_of(t * channels, channels), channels)
                here = pl.ds(pl.multiple_of((8 - t) * channels, channels), channels)
                w2t[there, :] = w2[here, :].T
                w1t[there, :] = w1[here, :].T

    order = [k for k in range(3 * shards // 4, shards)] + [k for k in range(1, 3 * shards // 4)]

    def peer_copy(kind, m, to, source, target):
        return pltpu.make_async_remote_copy(
            src_ref=source,
            dst_ref=target.at[m, me],
            send_sem=peer_send.at[kind, m],
            recv_sem=peer_recv.at[jnp.where(ahead, 0, 3) if kind == 0 else kind, m],
            device_id={"shard": to},
            device_id_type=MESH,
        )

    def send_units(m):
        for k in order:
            peer_copy(0, m, lax.rem(me + k, shards), unit_src.at[m], unit_all).start()

    def send_chosen(m):
        for k in order:
            to = lax.rem(me + k, shards)
            peer_copy(1, m, to, chosen_src.at[m, to], chosen_rcv).start()

    def send_sums(p, m, low, high, mine):
        def send(n):
            peer_copy(2, m, n, part_src.at[p, n], part_rcv).start()

        @pl.when(mine)
        def _():
            for k in range(1, high - low):
                send(low + lax.rem(me - low + k, high - low))
            part_rcv[m, me] = part_src[p, me]

        @pl.when(jnp.logical_not(mine))
        def _():
            for n in range(low, high):
                send(n)

    def arrivals(kind, m, target, count, sem):
        others = target.at[m, pl.ds(0, count)]
        return pltpu.make_async_remote_copy(
            src_ref=others,
            dst_ref=others,
            send_sem=peer_send.at[kind, m],
            recv_sem=peer_recv.at[sem, m],
            device_id={"shard": lax.rem(me + 1, shards)},
            device_id_type=MESH,
        )

    def units_from(m, sem, members, mine):
        @pl.when(mine)
        def _():
            if members > 1:
                arrivals(0, m, unit_all, members - 1, sem).wait_recv()

        @pl.when(jnp.logical_not(mine))
        def _():
            arrivals(0, m, unit_all, members, sem).wait_recv()

    def x_send(m, part, step=1):
        window = pl.ds(*parts[part])
        return pltpu.make_async_remote_copy(
            src_ref=xsend.at[m, window],
            dst_ref=xin.at[m, window],
            send_sem=xs_send.at[m, part],
            recv_sem=xs_recv.at[m, part],
            device_id={"section": section + step},
            device_id_type=MESH,
        )

    def g_send(m, part, step=-1):
        window = pl.ds(*parts[part])
        return pltpu.make_async_remote_copy(
            src_ref=gout.at[m, window],
            dst_ref=gin.at[m, window],
            send_sem=gs_send.at[m, part],
            recv_sem=gs_recv.at[m, part],
            device_id={"section": section + step},
            device_id_type=MESH,
        )

    def receive(copy, m, step, landing):
        for part in range(2):
            copy(m, part, step).wait_recv()
        spread_in(landing.at[m])

    def forward(m, finish, between=None):
        gain = gain_ref[...]
        bias = bias_ref[...]
        leak = leak_ref[...]
        half = (0.5 * (1.0 - leak)) * gain
        base = leak * gain + half
        quarter = 0.25 * (1.0 - leak)
        for start, count, total in conv(cols_a, w1, half_rows + STRIDE):
            z = total * gain + bias
            turn = jnp.tanh(z + z)
            share = base + half * turn
            active = jnp.maximum(z, leak * z) - quarter * jnp.log(0.5 + 0.5 * jnp.abs(turn))
            mask = keep[:count]
            for h in range(folds):
                slope[m, pl.ds(start, count), lanes(h)] = jnp.where(mask, share[:, lanes(h)], 0.0)
                padded[h, pl.ds(STRIDE + start, count), :] = jnp.where(mask, active[:, lanes(h)], 0.0)
            shift_cols(start, count)
        if between is not None:
            between()
        for part, (start, count, total) in enumerate(list(conv(cols_b, w2, half_rows))):
            finish(part, start, centre_of(start, count) + total)

    def backward(m, finish):
        for start, count, total in conv(cols_a, w2t, half_rows + STRIDE):
            hidden = total * slope[m, pl.ds(start, count), :]
            for h in range(folds):
                padded[h, pl.ds(STRIDE + start, count), :] = hidden[:, lanes(h)]
            shift_cols(start, count)
        for part, (start, count, total) in enumerate(list(conv(cols_b, w1t, half_rows))):
            finish(part, start, centre_of(start, count) + total)

    def small_waits():
        gain_copy.wait()
        bias_copy.wait()
        leak_copy.wait()

    @pl.when(section < sections - 1)
    def _():
        @pl.when(first)
        def _():
            with jax.named_scope("w_wait"):
                x_copy.wait()
            xall[...] = xraw[...].astype(f32)

        small_waits()
        with jax.named_scope("w_wait"):
            w1_copy.wait()

        def run(m, peeled):
            @pl.when(first)
            def _():
                for h in range(folds):
                    spread[h, pl.ds(GUARD, positions), :] = xall[
                        pl.ds(h * images + m, positions, stride=folds * images), :
                    ]

            @pl.when(section > 0)
            def _():
                receive(x_send, m, -1, xin)

            expand_cols()

            def finish(part, start, value):
                compact(start, value)
                packed_out(xsend.at[m], part)
                if peeled and part == 0:
                    greet()
                x_send(m, part).start()

            forward(m, finish, w2_copy.wait if peeled else None)

        with jax.named_scope("forward"):
            run(0, True)

        @pl.loop(1, images)
        def _(m):
            with jax.named_scope("forward"):
                run(m, False)

        flip()

        @pl.loop(0, images)
        def _(m):
            with jax.named_scope("g_wait"):
                for part in range(2):
                    g_send(m, part, 1).wait_recv()
            with jax.named_scope("backward"):
                spread_in(gin.at[m])
                expand_cols()

                def finish(part, start, value):
                    compact(start, value)
                    collect(m, start, value)

                backward(m, finish)

                @pl.when(section > 0)
                def _():
                    for part in range(2):
                        packed_out(gout.at[m], part)
                        g_send(m, part).start()

    @pl.when(last)
    def _():
        labels_copy.wait()
        offset_copy.wait()
        micro = labels_ref.shape[0]
        local = images // micro
        row = lax.broadcasted_iota(jnp.int32, (shards, labels_ref.shape[1]), 0)
        lane = lax.broadcasted_iota(jnp.int32, (shards, labels_ref.shape[1]), 1)
        wanted_by = []
        for m in range(micro):
            values = labels_ref[pl.ds(m, 1), :].astype(f32)
            for f in range(local):
                mine = jnp.where(lane == row * local + f, values, 0.0)
                wanted_by.append(jnp.sum(mine, axis=1, keepdims=True))
        front = lax.broadcasted_iota(jnp.int32, (shards, 1), 0) < lead
        for p in range(steps):
            early = wanted_by[min(p, images - 1)]
            label_col[pl.ds(p * shards, shards), :] = jnp.where(front, early, wanted_by[max(p - 1, 0)])
        ids = lax.broadcasted_iota(jnp.int32, (faces, class_count), 1)
        wanted = label_col[...].astype(jnp.int32) - offset_ref[0]
        hits[...] = jnp.where(wanted == ids, 1.0, 0.0).astype(bf16)

        depth_copy.wait()
        spread_in(depth)

        def store(i, d, h, value):
            dws[d + 1, pl.ds(STRIDE * i, STRIDE), pl.ds(LANES * h, LANES)] = value

        expand(store)
        with jax.named_scope("centre_wait"):
            centre_copy.wait()
        block = LANES

        @pl.loop(0, class_count // block, unroll=True)
        def _(b):
            part = pl.ds(pl.multiple_of(b * block, block), block)
            values = raw[part, :].astype(f32)
            square = jnp.mean(values * values, axis=-1, keepdims=True)
            factor = lax.rsqrt(square + tiny_value) / math.sqrt(width)
            normed = (values * factor).astype(bf16)
            centres[part, :] = normed
            centres_t[:, part] = normed.T

        picked[...] = dot(hits[...], centres[...])
        for m in range(images):
            for k in range(lines):
                chosen_src[m, pl.ds(0, lead), k, :] = picked[pl.ds(m * shards, lead), lanes(k)]
                chosen_src[m, pl.ds(lead, shards - lead), k, :] = picked[
                    pl.ds((m + 1) * shards + lead, shards - lead), lanes(k)
                ]
            chosen_rcv[m, me] = chosen_src[m, me]
        flat[...] = jnp.zeros_like(flat)
        embed_copy.wait()
        embed_t[...] = embed[...].T
        small_waits()
        with jax.named_scope("w_wait"):
            w1_copy.wait()
            w2_copy.wait()
        flip()
        greet()

        @pl.loop(0, images)
        def _(m):
            send_chosen(m)

        def last_forward(m):
            with jax.named_scope("x_wait"):
                receive(x_send, m, -1, xin)
            expand_cols()
            sums = []

            def finish(part, start, value):
                weighted = value.astype(bf16).astype(f32) * dws[1, pl.ds(start, value.shape[0]), :]
                sums.append(jnp.sum(weighted, axis=0, keepdims=True))

            forward(m, finish)
            pooled = jnp.broadcast_to(sums[0] + sums[1], (HALF_ROWS, channels)).astype(bf16)
            embedded = dot(pooled, embed[...])[:1]
            square = jnp.mean(embedded * embedded, axis=-1, keepdims=True)
            factor = lax.rsqrt(square + tiny_value) / math.sqrt(width)
            normed = (embedded * factor).astype(bf16).astype(f32)
            for k in range(lines):
                unit_src[m, pl.ds(k, 1), :] = normed[:, lanes(k)]
            unit_all[m, me] = unit_src[m]
            send_units(m)
            for k in range(lines):
                emb[m, pl.ds(k, 1), :] = embedded[:, lanes(k)]
            scales[m, pl.ds(0, 1), :] = jnp.broadcast_to(factor, (1, LANES))
            scales[m, pl.ds(1, 1), :] = jnp.broadcast_to(1.0 / (width * (square + tiny_value)), (1, LANES))

        def partial(p):
            with jax.named_scope("unit_wait"):

                @pl.when(p < images)
                def _():
                    units_from(p, 0, lead, ahead)
                    for k in range(lines):
                        flat[pl.ds(0, lead), lanes(k)] = unit_all[p, pl.ds(0, lead), k, :]

                @pl.when(p > 0)
                def _():
                    units_from(p - 1, 3, shards - lead, jnp.logical_not(ahead))
                    for k in range(lines):
                        flat[pl.ds(lead, shards - lead), lanes(k)] = unit_all[
                            p - 1, pl.ds(lead, shards - lead), k, :
                        ]

            cosines = dot(flat[...].astype(bf16), centres_t[...])
            mine = pl.ds(pl.multiple_of(p * shards, shards), shards)
            logits = scale_value * (cosines - margin_value * hits[mine, :].astype(f32))
            grown = jnp.exp(logits)
            weighted = dot(grown.astype(bf16), centres[...])
            for k in range(lines):
                part_src[p, :, k, :] = weighted[:, lanes(k)]
            part_src[p, :, lines, :] = jnp.broadcast_to(
                jnp.sum(grown, axis=1, keepdims=True), (shards, LANES)
            )

            @pl.when(p < images)
            def _():
                send_sums(p, p, 0, lead, ahead)

            @pl.when(p > 0)
            def _():
                send_sums(p, p - 1, lead, shards, jnp.logical_not(ahead))

        def last_backward(m):
            with jax.named_scope("chosen_wait"):
                arrivals(1, m, chosen_rcv, shards - 1, 1).wait_recv()
            chosen = jnp.sum(chosen_rcv[m], axis=0)
            with jax.named_scope("part_wait"):
                arrivals(2, m, part_rcv, shards - 1, 2).wait_recv()
            sums = jnp.sum(part_rcv[m], axis=0)
            grad_unit = scale_value * (sums[:lines] / sums[lines : lines + 1] - chosen)
            embedded = emb[m]
            factor = scales[m, 0:1, :]
            shrink = scales[m, 1:2, :]
            inner = jnp.sum(embedded * grad_unit, axis=0, keepdims=True)
            inner = jnp.sum(inner, axis=1, keepdims=True)
            grad_embed = factor * (grad_unit - embedded * (inner * shrink))
            grad_embed = jnp.concatenate(
                [jnp.broadcast_to(grad_embed[k : k + 1], (HALF_ROWS, LANES)) for k in range(lines)], axis=1
            ).astype(bf16)
            gpool = dot(grad_embed, embed_t[...])[:1]
            for d in range(3):
                cols_a[body, pl.ds(channels * d, channels)] = (gpool * dws[d]).astype(bf16)

            def finish(part, start, value):
                compact(start, value)
                packed_out(gout.at[m], part)
                g_send(m, part).start()
                collect(m, start, value)

            backward(m, finish)

        lag = 4

        def steps_done(t):
            late = me >= shards // 2
            lead_done = jnp.where(t < 1, 0, jnp.where(t < images - 1, 1, jnp.where(t < images + 1, 2, t - 1)))
            rest_done = jnp.where((t == 0) & late, 1, t)
            return jnp.clip(jnp.where(ahead, lead_done, rest_done), 0, steps)

        @pl.loop(0, images + lag)
        def _(t):
            @pl.when(t < images)
            def _():
                with jax.named_scope("forward"):
                    last_forward(t)

            @pl.loop(steps_done(t - 1), steps_done(t))
            def _(p):
                with jax.named_scope("partial"):
                    partial(p)

            @pl.when(t >= lag)
            def _():
                with jax.named_scope("backward"):
                    last_backward(t - lag)

    with jax.named_scope("drain"):
        out_ref[...] = oall[pl.ds(0, positions * folds * images), :].astype(bf16)

        @pl.loop(0, images)
        def _(m):
            for part in range(2):

                @pl.when(section < sections - 1)
                def _():
                    x_send(m, part).wait_send()

                @pl.when(section > 0)
                def _():
                    g_send(m, part).wait_send()

        @pl.when(last)
        def _():
            @pl.loop(0, images)
            def _(m):
                arrivals(0, m, unit_all, shards - 1, 0).wait_send()
                arrivals(1, m, chosen_rcv, shards - 1, 1).wait_send()
                arrivals(2, m, part_rcv, shards - 1, 2).wait_send()


def emit(source, target, sem):
    copy = pltpu.make_async_copy(source, target, sem)
    copy.start()
    copy.wait()


def on_device(
    section_input,
    conv_one,
    conv_two,
    unit_gain,
    offset_bias,
    leak_slope,
    depthwise,
    embed_weight,
    class_centers,
    labels,
    class_offsets,
):
    sections = lax.axis_size("section")
    shards = lax.axis_size("shard")
    micro, local, positions, channels = section_input.shape
    side = math.isqrt(positions)
    images = micro * local
    rows = side * STRIDE
    folds = channels // LANES
    width = embed_weight.shape[1]
    lines = width // LANES
    classes = class_centers.shape[0]
    faces = shards * (images + 1)
    hbm = pl.BlockSpec(memory_space=pltpu.HBM)
    vmem = pl.BlockSpec(memory_space=pltpu.VMEM)
    dma = pltpu.SemaphoreType.DMA
    vm = pltpu.VMEM
    lined = (positions * folds * images, LANES)
    taller = -(-(positions + STRIDE - side) // 8) * 8
    maps = vm((images, taller, channels), bf16)
    weights = vm(conv_one.shape[1:], bf16)
    columns = vm((rows + 2 * STRIDE, 3 * channels), bf16)
    row = vm((1, channels), f32)
    result = pl.pallas_call(
        functools.partial(kernel, sections, shards, images, side),
        out_shape=vm(lined, bf16),
        in_specs=[hbm] * 11,
        out_specs=vmem,
        scratch_shapes=[
            vm(lined, bf16),
            vm(lined, f32),
            maps,
            maps,
            maps,
            maps,
            vm(((positions + STRIDE - side) * folds * images, LANES), f32),
            weights,
            weights,
            weights,
            weights,
            row,
            row,
            row,
            vm((positions, channels), bf16),
            vm(embed_weight.shape, bf16),
            vm((width, channels), bf16),
            vm((classes, width), bf16),
            vm((classes, width), bf16),
            vm((width, classes), bf16),
            vm(labels.shape, jnp.int32),
            pltpu.SMEM(class_offsets.shape, jnp.int32),
            columns,
            columns,
            vm((folds, GUARD + -(-positions // 8) * 8 + 8, LANES), f32),
            vm((folds, rows + 2 * STRIDE, LANES), f32),
            vm((folds, taller, LANES), f32),
            vm((3, rows, channels), f32),
            vm((images, rows, channels), f32),
            vm((images, lines, LANES), f32),
            vm((images, 8, LANES), f32),
            vm((images, lines, LANES), f32),
            vm((images, shards, lines, LANES), f32),
            vm((shards, width), f32),
            vm((faces, 1), f32),
            vm((faces, classes), bf16),
            vm((faces, width), f32),
            vm((images, shards, lines, LANES), f32),
            vm((images, shards, lines, LANES), f32),
            vm((images + 1, shards, lines + 1, LANES), f32),
            vm((images, shards, lines + 1, LANES), f32),
            dma((11,)),
            dma((images, 2)),
            dma((images, 2)),
            dma((images, 2)),
            dma((images, 2)),
            dma((3, images)),
            dma((4, images)),
        ],
        compiler_params=pltpu.CompilerParams(
            collective_id=0, has_side_effects=True, vmem_limit_bytes=60000 * 1024
        ),
        name="window",
    )(
        section_input.reshape(images, positions, folds, LANES).transpose(1, 2, 0, 3).reshape(lined),
        conv_one,
        conv_two,
        unit_gain,
        offset_bias,
        leak_slope,
        depthwise,
        embed_weight,
        class_centers,
        labels,
        class_offsets,
    )
    result = pl.pallas_call(
        emit,
        out_shape=jax.ShapeDtypeStruct(lined, bf16),
        in_specs=[vmem],
        out_specs=hbm,
        scratch_shapes=[dma],
        name="emit",
    )(pltpu.with_memory_space_constraint(result, pltpu.VMEM))
    result = result.reshape(positions, folds, images, LANES).transpose(2, 0, 1, 3)
    return result.reshape(1, micro, local, positions, channels)


def solution(mesh):
    placed = (
        P(None, "shard", None, None),
        P("section", None, None),
        P("section", None, None),
        P("section", None),
        P("section", None),
        P("section", None),
        P(),
        P(),
        P("shard", None),
        P(),
        P("shard"),
    )
    return jax.shard_map(
        on_device,
        mesh=mesh,
        in_specs=placed,
        out_specs=P("section", None, "shard", None, None),
        check_vma=False,
    )
```

```python
import functools
import math

import jax
import jax.numpy as jnp
from jax import lax
from jax.experimental import pallas as pl
from jax.experimental.pallas import tpu as pltpu
from jax.sharding import PartitionSpec as P

MESH = pl.DeviceIdType.MESH
STRIDE = 16
GUARD = 16
HALF_ROWS = 16
LANES = 128

margin_value = 0.4
scale_value = 64.0
tiny_value = 1e-06
lowest = -3e38

f32 = jnp.float32
bf16 = jnp.bfloat16


def dot(left, right):
    return jnp.dot(left, right, preferred_element_type=f32)


def kernel(
    sections,
    shards,
    images,
    side,
    x_hbm,
    w1_hbm,
    w2_hbm,
    gain_hbm,
    bias_hbm,
    leak_hbm,
    depth_hbm,
    embed_hbm,
    centre_hbm,
    labels_hbm,
    offset_hbm,
    out_ref,
    xraw,
    xall,
    xin,
    xsend,
    gin,
    gout,
    oall,
    w1,
    w2,
    w1t,
    w2t,
    gain_ref,
    bias_ref,
    leak_ref,
    depth,
    embed,
    embed_t,
    raw,
    centres,
    centres_t,
    labels_ref,
    offset_ref,
    cols_a,
    cols_b,
    spread,
    padded,
    packed,
    dws,
    slope,
    emb,
    scales,
    unit_src,
    unit_all,
    flat,
    label_col,
    hits,
    picked,
    chosen_src,
    chosen_rcv,
    part_src,
    part_rcv,
    in_sem,
    xs_send,
    xs_recv,
    gs_send,
    gs_recv,
    peer_send,
    peer_recv,
):
    section = lax.axis_index("section")
    me = lax.axis_index("shard")
    first = section == 0
    last = section == sections - 1
    positions = side * side
    rows = side * STRIDE
    channels = w1.shape[1]
    folds = channels // LANES
    width = embed.shape[1]
    lines = width // LANES
    class_count = centres.shape[0]
    lead = max(shards // 8, 1)
    steps = images + 1
    ahead = me < lead
    faces = steps * shards
    body = pl.ds(STRIDE, rows)

    def bring(k, source, target):
        return pltpu.make_async_copy(source, target, in_sem.at[k])

    x_copy = bring(0, x_hbm, xraw)
    w1_copy = bring(1, w1_hbm.at[0], w1)
    w2_copy = bring(2, w2_hbm.at[0], w2)
    gain_copy = bring(3, gain_hbm, gain_ref)
    bias_copy = bring(4, bias_hbm, bias_ref)
    leak_copy = bring(5, leak_hbm, leak_ref)
    depth_copy = bring(6, depth_hbm, depth)
    embed_copy = bring(7, embed_hbm, embed)
    centre_copy = bring(8, centre_hbm, raw)
    labels_copy = bring(9, labels_hbm, labels_ref)
    offset_copy = bring(10, offset_hbm, offset_ref)

    @pl.when(first)
    def _():
        x_copy.start()

    @pl.when(last)
    def _():
        labels_copy.start()
        offset_copy.start()
        depth_copy.start()
        centre_copy.start()

    w1_copy.start()
    gain_copy.start()
    bias_copy.start()
    leak_copy.start()
    w2_copy.start()

    @pl.when(last)
    def _():
        embed_copy.start()

    barrier = pltpu.get_barrier_semaphore()

    @pl.when(section > 0)
    def _():
        pl.semaphore_signal(barrier, inc=1, device_id={"section": section - 1}, device_id_type=MESH)

    @pl.when(section < sections - 1)
    def _():
        pl.semaphore_signal(barrier, inc=1, device_id={"section": section + 1}, device_id_type=MESH)

    @pl.when(last)
    def _():
        for k in range(1, shards):
            peer = lax.rem(me + k, shards)
            pl.semaphore_signal(barrier, inc=1, device_id={"shard": peer}, device_id_type=MESH)

    neighbours = jnp.where(first, 0, 1) + jnp.where(last, shards - 1, 1)

    def greet():
        with jax.named_scope("barrier"):
            pl.semaphore_wait(barrier, neighbours)

    for cols in (cols_a, cols_b):
        cols[pl.ds(0, STRIDE), :] = jnp.zeros((STRIDE, 3 * channels), bf16)
        cols[pl.ds(rows + STRIDE, STRIDE), :] = jnp.zeros((STRIDE, 3 * channels), bf16)
    for h in range(folds):
        padded[h, pl.ds(0, STRIDE), :] = jnp.zeros((STRIDE, LANES), f32)
        padded[h, pl.ds(rows + STRIDE, STRIDE), :] = jnp.zeros((STRIDE, LANES), f32)
        spread[h, pl.ds(0, GUARD), :] = jnp.zeros((GUARD, LANES), f32)
        tail = spread.shape[1] - GUARD - positions
        spread[h, pl.ds(GUARD + positions, tail), :] = jnp.zeros((tail, LANES), f32)
        packed[h, pl.ds(packed.shape[1] - 8, 8), :] = jnp.zeros((8, LANES), f32)

    column = lax.broadcasted_iota(jnp.int32, (STRIDE, LANES), 0)
    inside = {
        -1: (column >= 1) & (column < side),
        0: column < side,
        1: column < side - 1,
    }
    keep = (lax.broadcasted_iota(jnp.int32, (rows, LANES), 0) & (STRIDE - 1)) < side

    def lanes(h):
        return slice(h * LANES, (h + 1) * LANES)

    def spread_in(source):
        for h in range(folds):
            spread[h, pl.ds(GUARD, positions), :] = source[pl.ds(0, positions), lanes(h)].astype(f32)

    def expand(store):
        for i in range(side):
            for d in (-1, 0, 1):
                for h in range(folds):
                    value = spread[h, pl.ds(GUARD + side * i + d, STRIDE), :]
                    store(i, d, h, jnp.where(inside[d], value, 0.0))

    def expand_cols():
        def store(i, d, h, value):
            target = pl.ds(channels * (d + 1) + LANES * h, LANES)
            cols_a[pl.ds(STRIDE * (i + 1), STRIDE), target] = value.astype(bf16)

        expand(store)

    def shift_cols(start, count):
        for h in range(folds):
            for d in (-1, 0, 1):
                target = pl.ds(channels * (d + 1) + LANES * h, LANES)
                source = padded[h, pl.ds(STRIDE + start + d, count), :]
                cols_b[pl.ds(STRIDE + start, count), target] = source.astype(bf16)

    def centre_of(start, count):
        return cols_a[pl.ds(STRIDE + start, count), pl.ds(channels, channels)].astype(f32)

    depth3 = 3 * channels

    def chain(cols, weights, start, count, taps):
        total = None
        for d in range(3):
            low, high = max(taps[0] - 3 * d, 0), min(taps[1] - 3 * d, 3)
            if low < high:
                left = cols[pl.ds(start + STRIDE * d, count), pl.ds(channels * low, channels * (high - low))]
                right = weights[pl.ds(depth3 * d + channels * low, channels * (high - low)), :]
                term = dot(left, right)
                total = term if total is None else total + term
        return total

    def conv(cols, weights, cut):
        for start, count, middle in ((0, cut, 5), (cut, rows - cut, 4)):
            one = chain(cols, weights, start, count, (0, middle))
            two = chain(cols, weights, start, count, (middle, 9))
            yield start, count, one + jnp.maximum(two, lowest)

    half_rows = side // 2 * STRIDE
    send_cut = side // 2 * side // 8 * 8
    parts = ((0, send_cut), (send_cut, positions - send_cut))

    def compact(start, value):
        for i in range(value.shape[0] // STRIDE):
            for h in range(folds):
                piece = value[STRIDE * i : STRIDE * (i + 1), lanes(h)]
                packed[h, pl.ds(side * (start // STRIDE + i), STRIDE), :] = piece

    def collect(m, start, value):
        for i in range(value.shape[0] // STRIDE):
            for h in range(folds):
                piece = value[STRIDE * i : STRIDE * (i + 1), lanes(h)]
                where = (side * (start // STRIDE + i) * folds + h) * images + m
                oall[pl.ds(where, STRIDE, stride=folds * images), :] = piece

    def packed_out(target, part):
        low, count = parts[part]
        for h in range(folds):
            target[pl.ds(low, count), pl.ds(LANES * h, LANES)] = packed[h, pl.ds(low, count), :].astype(bf16)

    def flip():
        with jax.named_scope("flip"):

            @pl.loop(0, 9)
            def _(t):
                there = pl.ds(pl.multiple_of(t * channels, channels), channels)
                here = pl.ds(pl.multiple_of((8 - t) * channels, channels), channels)
                w2t[there, :] = w2[here, :].T
                w1t[there, :] = w1[here, :].T

    order = [k for k in range(3 * shards // 4, shards)] + [k for k in range(1, 3 * shards // 4)]

    def peer_copy(kind, m, to, source, target):
        return pltpu.make_async_remote_copy(
            src_ref=source,
            dst_ref=target.at[m, me],
            send_sem=peer_send.at[kind, m],
            recv_sem=peer_recv.at[jnp.where(ahead, 0, 3) if kind == 0 else kind, m],
            device_id={"shard": to},
            device_id_type=MESH,
        )

    def send_units(m):
        for k in order:
            peer_copy(0, m, lax.rem(me + k, shards), unit_src.at[m], unit_all).start()

    def send_chosen(m):
        for k in order:
            to = lax.rem(me + k, shards)
            peer_copy(1, m, to, chosen_src.at[m, to], chosen_rcv).start()

    def send_sums(p, m, low, high, mine):
        def send(n):
            peer_copy(2, m, n, part_src.at[p, n], part_rcv).start()

        @pl.when(mine)
        def _():
            for k in range(1, high - low):
                send(low + lax.rem(me - low + k, high - low))
            part_rcv[m, me] = part_src[p, me]

        @pl.when(jnp.logical_not(mine))
        def _():
            for n in range(low, high):
                send(n)

    def arrivals(kind, m, target, count, sem):
        others = target.at[m, pl.ds(0, count)]
        return pltpu.make_async_remote_copy(
            src_ref=others,
            dst_ref=others,
            send_sem=peer_send.at[kind, m],
            recv_sem=peer_recv.at[sem, m],
            device_id={"shard": lax.rem(me + 1, shards)},
            device_id_type=MESH,
        )

    def units_from(m, sem, members, mine):
        @pl.when(mine)
        def _():
            if members > 1:
                arrivals(0, m, unit_all, members - 1, sem).wait_recv()

        @pl.when(jnp.logical_not(mine))
        def _():
            arrivals(0, m, unit_all, members, sem).wait_recv()

    def x_send(m, part, step=1):
        window = pl.ds(*parts[part])
        return pltpu.make_async_remote_copy(
            src_ref=xsend.at[m, window],
            dst_ref=xin.at[m, window],
            send_sem=xs_send.at[m, part],
            recv_sem=xs_recv.at[m, part],
            device_id={"section": section + step},
            device_id_type=MESH,
        )

    def g_send(m, part, step=-1):
        window = pl.ds(*parts[part])
        return pltpu.make_async_remote_copy(
            src_ref=gout.at[m, window],
            dst_ref=gin.at[m, window],
            send_sem=gs_send.at[m, part],
            recv_sem=gs_recv.at[m, part],
            device_id={"section": section + step},
            device_id_type=MESH,
        )

    def receive(copy, m, step, landing):
        for part in range(2):
            copy(m, part, step).wait_recv()
        spread_in(landing.at[m])

    def forward(m, finish, between=None):
        gain = gain_ref[...]
        bias = bias_ref[...]
        leak = leak_ref[...]
        half = (0.5 * (1.0 - leak)) * gain
        base = leak * gain + half
        quarter = 0.25 * (1.0 - leak)
        for start, count, total in conv(cols_a, w1, half_rows + STRIDE):
            z = total * gain + bias
            turn = jnp.tanh(z + z)
            share = base + half * turn
            active = jnp.maximum(z, leak * z) - quarter * jnp.log(0.5 + 0.5 * jnp.abs(turn))
            mask = keep[:count]
            for h in range(folds):
                slope[m, pl.ds(start, count), lanes(h)] = jnp.where(mask, share[:, lanes(h)], 0.0)
                padded[h, pl.ds(STRIDE + start, count), :] = jnp.where(mask, active[:, lanes(h)], 0.0)
            shift_cols(start, count)
        if between is not None:
            between()
        for part, (start, count, total) in enumerate(list(conv(cols_b, w2, half_rows))):
            finish(part, start, centre_of(start, count) + total)

    def backward(m, finish):
        for start, count, total in conv(cols_a, w2t, half_rows + STRIDE):
            hidden = total * slope[m, pl.ds(start, count), :]
            for h in range(folds):
                padded[h, pl.ds(STRIDE + start, count), :] = hidden[:, lanes(h)]
            shift_cols(start, count)
        for part, (start, count, total) in enumerate(list(conv(cols_b, w1t, half_rows))):
            finish(part, start, centre_of(start, count) + total)

    def small_waits():
        gain_copy.wait()
        bias_copy.wait()
        leak_copy.wait()

    @pl.when(section < sections - 1)
    def _():
        @pl.when(first)
        def _():
            with jax.named_scope("w_wait"):
                x_copy.wait()
            xall[...] = xraw[...].astype(f32)

        small_waits()
        with jax.named_scope("w_wait"):
            w1_copy.wait()

        def run(m, peeled):
            @pl.when(first)
            def _():
                for h in range(folds):
                    spread[h, pl.ds(GUARD, positions), :] = xall[
                        pl.ds(h * images + m, positions, stride=folds * images), :
                    ]

            @pl.when(section > 0)
            def _():
                receive(x_send, m, -1, xin)

            expand_cols()

            def finish(part, start, value):
                compact(start, value)
                packed_out(xsend.at[m], part)
                if peeled and part == 0:
                    greet()
                x_send(m, part).start()

            forward(m, finish, w2_copy.wait if peeled else None)

        with jax.named_scope("forward"):
            run(0, True)

        @pl.loop(1, images)
        def _(m):
            with jax.named_scope("forward"):
                run(m, False)

        flip()

        @pl.loop(0, images)
        def _(m):
            with jax.named_scope("g_wait"):
                for part in range(2):
                    g_send(m, part, 1).wait_recv()
            with jax.named_scope("backward"):
                spread_in(gin.at[m])
                expand_cols()

                def finish(part, start, value):
                    compact(start, value)
                    collect(m, start, value)

                backward(m, finish)

                @pl.when(section > 0)
                def _():
                    for part in range(2):
                        packed_out(gout.at[m], part)
                        g_send(m, part).start()

    @pl.when(last)
    def _():
        labels_copy.wait()
        offset_copy.wait()
        micro = labels_ref.shape[0]
        local = images // micro
        row = lax.broadcasted_iota(jnp.int32, (shards, labels_ref.shape[1]), 0)
        lane = lax.broadcasted_iota(jnp.int32, (shards, labels_ref.shape[1]), 1)
        wanted_by = []
        for m in range(micro):
            values = labels_ref[pl.ds(m, 1), :].astype(f32)
            for f in range(local):
                mine = jnp.where(lane == row * local + f, values, 0.0)
                wanted_by.append(jnp.sum(mine, axis=1, keepdims=True))
        front = lax.broadcasted_iota(jnp.int32, (shards, 1), 0) < lead
        for p in range(steps):
            early = wanted_by[min(p, images - 1)]
            label_col[pl.ds(p * shards, shards), :] = jnp.where(front, early, wanted_by[max(p - 1, 0)])
        ids = lax.broadcasted_iota(jnp.int32, (faces, class_count), 1)
        wanted = label_col[...].astype(jnp.int32) - offset_ref[0]
        hits[...] = jnp.where(wanted == ids, 1.0, 0.0).astype(bf16)

        depth_copy.wait()
        spread_in(depth)

        def store(i, d, h, value):
            dws[d + 1, pl.ds(STRIDE * i, STRIDE), pl.ds(LANES * h, LANES)] = value

        expand(store)
        with jax.named_scope("centre_wait"):
            centre_copy.wait()
        block = LANES

        @pl.loop(0, class_count // block, unroll=True)
        def _(b):
            part = pl.ds(pl.multiple_of(b * block, block), block)
            values = raw[part, :].astype(f32)
            square = jnp.mean(values * values, axis=-1, keepdims=True)
            factor = lax.rsqrt(square + tiny_value) / math.sqrt(width)
            normed = (values * factor).astype(bf16)
            centres[part, :] = normed
            centres_t[:, part] = normed.T

        picked[...] = dot(hits[...], centres[...])
        for m in range(images):
            for k in range(lines):
                chosen_src[m, pl.ds(0, lead), k, :] = picked[pl.ds(m * shards, lead), lanes(k)]
                chosen_src[m, pl.ds(lead, shards - lead), k, :] = picked[
                    pl.ds((m + 1) * shards + lead, shards - lead), lanes(k)
                ]
            chosen_rcv[m, me] = chosen_src[m, me]
        flat[...] = jnp.zeros_like(flat)
        embed_copy.wait()
        embed_t[...] = embed[...].T
        small_waits()
        with jax.named_scope("w_wait"):
            w1_copy.wait()
            w2_copy.wait()
        flip()
        greet()

        @pl.loop(0, images)
        def _(m):
            send_chosen(m)

        def last_forward(m):
            with jax.named_scope("x_wait"):
                receive(x_send, m, -1, xin)
            expand_cols()
            sums = []

            def finish(part, start, value):
                weighted = value.astype(bf16).astype(f32) * dws[1, pl.ds(start, value.shape[0]), :]
                sums.append(jnp.sum(weighted, axis=0, keepdims=True))

            forward(m, finish)
            pooled = jnp.broadcast_to(sums[0] + sums[1], (HALF_ROWS, channels)).astype(bf16)
            embedded = dot(pooled, embed[...])[:1]
            square = jnp.mean(embedded * embedded, axis=-1, keepdims=True)
            factor = lax.rsqrt(square + tiny_value) / math.sqrt(width)
            normed = (embedded * factor).astype(bf16).astype(f32)
            for k in range(lines):
                unit_src[m, pl.ds(k, 1), :] = normed[:, lanes(k)]
            unit_all[m, me] = unit_src[m]
            send_units(m)
            for k in range(lines):
                emb[m, pl.ds(k, 1), :] = embedded[:, lanes(k)]
            scales[m, pl.ds(0, 1), :] = jnp.broadcast_to(factor, (1, LANES))
            scales[m, pl.ds(1, 1), :] = jnp.broadcast_to(1.0 / (width * (square + tiny_value)), (1, LANES))

        def partial(p):
            with jax.named_scope("unit_wait"):

                @pl.when(p < images)
                def _():
                    units_from(p, 0, lead, ahead)
                    for k in range(lines):
                        flat[pl.ds(0, lead), lanes(k)] = unit_all[p, pl.ds(0, lead), k, :]

                @pl.when(p > 0)
                def _():
                    units_from(p - 1, 3, shards - lead, jnp.logical_not(ahead))
                    for k in range(lines):
                        flat[pl.ds(lead, shards - lead), lanes(k)] = unit_all[
                            p - 1, pl.ds(lead, shards - lead), k, :
                        ]

            cosines = dot(flat[...].astype(bf16), centres_t[...])
            mine = pl.ds(pl.multiple_of(p * shards, shards), shards)
            logits = scale_value * (cosines - margin_value * hits[mine, :].astype(f32))
            grown = jnp.exp(logits)
            weighted = dot(grown.astype(bf16), centres[...])
            for k in range(lines):
                part_src[p, :, k, :] = weighted[:, lanes(k)]
            part_src[p, :, lines, :] = jnp.broadcast_to(
                jnp.sum(grown, axis=1, keepdims=True), (shards, LANES)
            )

            @pl.when(p < images)
            def _():
                send_sums(p, p, 0, lead, ahead)

            @pl.when(p > 0)
            def _():
                send_sums(p, p - 1, lead, shards, jnp.logical_not(ahead))

        def last_backward(m):
            with jax.named_scope("chosen_wait"):
                arrivals(1, m, chosen_rcv, shards - 1, 1).wait_recv()
            chosen = jnp.sum(chosen_rcv[m], axis=0)
            with jax.named_scope("part_wait"):
                arrivals(2, m, part_rcv, shards - 1, 2).wait_recv()
            sums = jnp.sum(part_rcv[m], axis=0)
            grad_unit = scale_value * (sums[:lines] / sums[lines : lines + 1] - chosen)
            embedded = emb[m]
            factor = scales[m, 0:1, :]
            shrink = scales[m, 1:2, :]
            inner = jnp.sum(embedded * grad_unit, axis=0, keepdims=True)
            inner = jnp.sum(inner, axis=1, keepdims=True)
            grad_embed = factor * (grad_unit - embedded * (inner * shrink))
            grad_embed = jnp.concatenate(
                [jnp.broadcast_to(grad_embed[k : k + 1], (HALF_ROWS, LANES)) for k in range(lines)], axis=1
            ).astype(bf16)
            gpool = dot(grad_embed, embed_t[...])[:1]
            for d in range(3):
                cols_a[body, pl.ds(channels * d, channels)] = (gpool * dws[d]).astype(bf16)

            def finish(part, start, value):
                compact(start, value)
                packed_out(gout.at[m], part)
                g_send(m, part).start()
                collect(m, start, value)

            backward(m, finish)

        lag = 4

        def steps_done(t):
            late = me >= shards // 2
            lead_done = jnp.where(t < 1, 0, jnp.where(t < images - 1, 1, jnp.where(t < images + 1, 2, t - 1)))
            rest_done = jnp.where((t == 0) & late, 1, t)
            return jnp.clip(jnp.where(ahead, lead_done, rest_done), 0, steps)

        @pl.loop(0, images + lag)
        def _(t):
            @pl.when(t < images)
            def _():
                with jax.named_scope("forward"):
                    last_forward(t)

            @pl.loop(steps_done(t - 1), steps_done(t))
            def _(p):
                with jax.named_scope("partial"):
                    partial(p)

            @pl.when(t >= lag)
            def _():
                with jax.named_scope("backward"):
                    last_backward(t - lag)

    with jax.named_scope("drain"):
        out_ref[...] = oall[pl.ds(0, positions * folds * images), :].astype(bf16)

        @pl.loop(0, images)
        def _(m):
            for part in range(2):

                @pl.when(section < sections - 1)
                def _():
                    x_send(m, part).wait_send()

                @pl.when(section > 0)
                def _():
                    g_send(m, part).wait_send()

        @pl.when(last)
        def _():
            @pl.loop(0, images)
            def _(m):
                arrivals(0, m, unit_all, shards - 1, 0).wait_send()
                arrivals(1, m, chosen_rcv, shards - 1, 1).wait_send()
                arrivals(2, m, part_rcv, shards - 1, 2).wait_send()


def emit(source, target, sem):
    copy = pltpu.make_async_copy(source, target, sem)
    copy.start()
    copy.wait()


def on_device(
    section_input,
    conv_one,
    conv_two,
    unit_gain,
    offset_bias,
    leak_slope,
    depthwise,
    embed_weight,
    class_centers,
    labels,
    class_offsets,
):
    sections = lax.axis_size("section")
    shards = lax.axis_size("shard")
    micro, local, positions, channels = section_input.shape
    side = math.isqrt(positions)
    images = micro * local
    rows = side * STRIDE
    folds = channels // LANES
    width = embed_weight.shape[1]
    lines = width // LANES
    classes = class_centers.shape[0]
    faces = shards * (images + 1)
    hbm = pl.BlockSpec(memory_space=pltpu.HBM)
    vmem = pl.BlockSpec(memory_space=pltpu.VMEM)
    dma = pltpu.SemaphoreType.DMA
    vm = pltpu.VMEM
    lined = (positions * folds * images, LANES)
    taller = -(-(positions + STRIDE - side) // 8) * 8
    maps = vm((images, positions, channels), bf16)
    weights = vm(conv_one.shape[1:], bf16)
    columns = vm((rows + 2 * STRIDE, 3 * channels), bf16)
    row = vm((1, channels), f32)
    result = pl.pallas_call(
        functools.partial(kernel, sections, shards, images, side),
        out_shape=vm(lined, bf16),
        in_specs=[hbm] * 11,
        out_specs=vmem,
        scratch_shapes=[
            vm(lined, bf16),
            vm(lined, f32),
            maps,
            maps,
            maps,
            maps,
            vm(((positions + STRIDE - side) * folds * images, LANES), f32),
            weights,
            weights,
            weights,
            weights,
            row,
            row,
            row,
            vm((positions, channels), bf16),
            vm(embed_weight.shape, bf16),
            vm((width, channels), bf16),
            vm((classes, width), bf16),
            vm((classes, width), bf16),
            vm((width, classes), bf16),
            vm(labels.shape, jnp.int32),
            pltpu.SMEM(class_offsets.shape, jnp.int32),
            columns,
            columns,
            vm((folds, GUARD + -(-positions // 8) * 8 + 8, LANES), f32),
            vm((folds, rows + 2 * STRIDE, LANES), f32),
            vm((folds, taller, LANES), f32),
            vm((3, rows, channels), f32),
            vm((images, rows, channels), f32),
            vm((images, lines, LANES), f32),
            vm((images, 8, LANES), f32),
            vm((images, lines, LANES), f32),
            vm((images, shards, lines, LANES), f32),
            vm((shards, width), f32),
            vm((faces, 1), f32),
            vm((faces, classes), bf16),
            vm((faces, width), f32),
            vm((images, shards, lines, LANES), f32),
            vm((images, shards, lines, LANES), f32),
            vm((images + 1, shards, lines + 1, LANES), f32),
            vm((images, shards, lines + 1, LANES), f32),
            dma((11,)),
            dma((images, 2)),
            dma((images, 2)),
            dma((images, 2)),
            dma((images, 2)),
            dma((3, images)),
            dma((4, images)),
        ],
        compiler_params=pltpu.CompilerParams(
            collective_id=0, has_side_effects=True, vmem_limit_bytes=60000 * 1024
        ),
        name="window",
    )(
        section_input.reshape(images, positions, folds, LANES).transpose(1, 2, 0, 3).reshape(lined),
        conv_one,
        conv_two,
        unit_gain,
        offset_bias,
        leak_slope,
        depthwise,
        embed_weight,
        class_centers,
        labels,
        class_offsets,
    )
    result = pl.pallas_call(
        emit,
        out_shape=jax.ShapeDtypeStruct(lined, bf16),
        in_specs=[vmem],
        out_specs=hbm,
        scratch_shapes=[dma],
        name="emit",
    )(pltpu.with_memory_space_constraint(result, pltpu.VMEM))
    result = result.reshape(positions, folds, images, LANES).transpose(2, 0, 1, 3)
    return result.reshape(1, micro, local, positions, channels)


def solution(mesh):
    placed = (
        P(None, "shard", None, None),
        P("section", None, None),
        P("section", None, None),
        P("section", None),
        P("section", None),
        P("section", None),
        P(),
        P(),
        P("shard", None),
        P(),
        P("shard"),
    )
    return jax.shard_map(
        on_device,
        mesh=mesh,
        in_specs=placed,
        out_specs=P("section", None, "shard", None, None),
        check_vma=False,
    )
```
